32 devices in a mesh: req: 8 (over y, x, core), head: 4 (over z).
Axes of the slice: x: 2, y: 2, z: 4, core: 2. Of those that a mesh axis runs over, the one named last changes fastest.
Arguments:
- queries: bfloat16 [128, 64, 128], P('req', 'head'), may hold values from -6 to 6
- k_codes: bfloat16 [8192, 16, 8, 128], P('req', None, 'head'), may hold values from -6 to 6
- value_quantized_codes: bfloat16 [8192, 16, 8, 128], P('req', None, 'head'), may hold values from -6 to 6
- key_page_scale: float32 [8192, 8], P('req', 'head'), may hold values from 0.5 to 2
- value_page_scale: float32 [8192, 8], P('req', 'head'), may hold values from 4 to 16
- lengths: int32 [128], P('req'), may hold values from 1 to 2032
- page_table: int32 [128, 128], P('req'), may hold values from -1 to 8191, as said below
- out_weight: bfloat16 [8192, 8192], P('head', 'req'), may hold values from -0.0625 to 0.0625
Outputs:
- attn_out: bfloat16 [128, 8192], P(None, ('req', 'head'))
The draws below stay inside these ranges and needn't reach their ends.
Inputs may be any that keep to these rules, and one draw needn't show every extreme that they name: `page_table`: entries j below ceil(lengths[r] / 16) name pool pages; all such entries of all requests together name every pool page exactly once. Entries beyond are -1.
All inputs are finite; a program needn't handle non-finite values.
Results may differ from the reference program's by a relative error of at most 0.02.
Values may be sent and summed in bfloat16 or wider, within the bound.
No kernel may reach another device: no remote copies, remote signals or barrier semaphores. Data moves between devices by JAX's collectives and lax.ppermute only.
A program may use at most 128 MiB of HBM per device.

```python
import math
import jax
import jax.numpy as jnp
from jax import lax

QUERY_HEADS = 64
KEY_VALUE_HEADS = 8
HEAD_DIMENSION = 128
DMODEL = 8192
PAGE_TOKENS = 16
MAXP = 128
R_DEV = 16
REQS = 128
POOL_PAGES = 8192
N_REQ = 8


def page_layout(key):
    half_count = REQS // 2
    middle = MAXP // 2
    sign_dev = 2 * jax.random.randint(jax.random.fold_in(key, 1), (N_REQ // 2,), 0, 2) - 1
    shift = jax.random.randint(jax.random.fold_in(key, 2), (half_count,), 0, middle)
    selected_pages = jax.random.randint(jax.random.fold_in(key, 3), (), 0, half_count)
    shift = shift.at[selected_pages].set(middle - 1)
    owner_dev = jnp.arange(half_count, dtype=jnp.int32) // R_DEV
    turned = sign_dev[owner_dev] * shift
    page_count = jnp.concatenate([middle + turned, middle - turned]).astype(jnp.int32)
    remainder = jax.random.randint(jax.random.fold_in(key, 4), (REQS,), 1, PAGE_TOKENS + 1)
    longest = jnp.where(sign_dev[selected_pages // R_DEV] > 0, selected_pages, selected_pages + half_count)
    remainder = remainder.at[longest].set(PAGE_TOKENS)
    lengths = ((page_count - 1) * PAGE_TOKENS + remainder).astype(jnp.int32)
    shuffled = jax.random.permutation(jax.random.fold_in(key, 5), POOL_PAGES).astype(jnp.int32)
    starts = jnp.cumsum(page_count) - page_count
    entry = jnp.arange(MAXP, dtype=jnp.int32)[None, :]
    slot = jnp.clip(starts[:, None] + entry, 0, POOL_PAGES - 1)
    table = jnp.where(entry < page_count[:, None], shuffled[slot], -1).astype(jnp.int32)
    return (lengths, table)


def draw_lengths(key, part):
    return page_layout(jax.random.fold_in(key, 11))[0]


def draw_page_table(key, part):
    return page_layout(jax.random.fold_in(key, 11))[1]


def draw_queries(key, part):
    value_rows = jnp.clip(jax.random.normal(jax.random.fold_in(key, 21), (REQS, QUERY_HEADS, HEAD_DIMENSION), jnp.float32), -6.0, 6.0)
    return value_rows.astype(jnp.bfloat16)


def draw_k_codes(key, part):
    value_rows = jnp.clip(jax.random.normal(jax.random.fold_in(key, 31), (POOL_PAGES, PAGE_TOKENS, KEY_VALUE_HEADS, HEAD_DIMENSION), jnp.float32), -6.0, 6.0)
    return value_rows.astype(jnp.bfloat16)


def steps_of(rng, extent, split, smallest, high):
    level = 1.0
    for dim, parts in split:
        draws = jax.random.uniform(jax.random.fold_in(jax.random.fold_in(rng, 6), dim), (parts,), jnp.float32, smallest / len(split), high / len(split))
        level = level * jnp.repeat(jnp.exp(draws), extent[dim] // parts).reshape((-1,) + (1,) * (len(extent) - 1 - dim))
    return level


def normal_values(key, extent, width, reach, shards=(), held_as=jnp.bfloat16):
    level = steps_of(key, extent, shards, -0.22, 0.18) if shards else 1.0
    array = jax.random.normal(key, extent, jnp.float32) * width * level
    return jnp.minimum(jnp.maximum(array, -reach), reach).astype(held_as)


def setup_inputs(seed: int = 0) -> dict:
    arg_keys = jax.random.split(jax.random.key(seed), 9)
    queries = draw_queries(jax.random.fold_in(arg_keys[8], 71), 0)
    k_codes = draw_k_codes(jax.random.fold_in(arg_keys[8], 71), 0)
    value_quantized_codes = normal_values(arg_keys[2], (POOL_PAGES, PAGE_TOKENS, KEY_VALUE_HEADS, HEAD_DIMENSION), 1.0, 6.0, ((0, 8), (2, 4)))
    key_page_scale = jnp.clip(jnp.exp(math.log(2.0) - 1.3862944 * jax.random.uniform(arg_keys[3], (POOL_PAGES, KEY_VALUE_HEADS), jnp.float32) ** steps_of(arg_keys[3], (POOL_PAGES, KEY_VALUE_HEADS), ((0, 8), (1, 4)), -0.2, 0.2)), 0.5, 2.0)
    value_page_scale = jnp.clip(jnp.exp(math.log(16.0) - 1.3862944 * jax.random.uniform(arg_keys[4], (POOL_PAGES, KEY_VALUE_HEADS), jnp.float32) ** steps_of(arg_keys[4], (POOL_PAGES, KEY_VALUE_HEADS), ((0, 8), (1, 4)), -0.2, 0.2)), 4.0, 16.0)
    lengths = draw_lengths(jax.random.fold_in(arg_keys[8], 71), 0)
    page_table = draw_page_table(jax.random.fold_in(arg_keys[8], 71), 0)
    out_weight = normal_values(arg_keys[7], (QUERY_HEADS * HEAD_DIMENSION, DMODEL), (QUERY_HEADS * HEAD_DIMENSION) ** -0.5, 0.0625, ((0, 4), (1, 8)))
    return {"queries": queries, "k_codes": k_codes, "value_quantized_codes": value_quantized_codes, "key_page_scale": key_page_scale, "value_page_scale": value_page_scale, "lengths": lengths, "page_table": page_table, "out_weight": out_weight}


floor_score = -1e+30

def reference(queries, k_codes, value_quantized_codes, key_page_scale, value_page_scale, lengths, page_table, out_weight):
    query_group_count = QUERY_HEADS // KEY_VALUE_HEADS

    def per_request(inputs_row):
        query_vector, length_row, table_row = inputs_row
        page_ids = jnp.maximum(table_row, 0).astype(jnp.int32)
        keys = k_codes[page_ids].astype(jnp.float32)
        value_rows = value_quantized_codes[page_ids].astype(jnp.float32)
        query_float = query_vector.astype(jnp.float32).reshape(KEY_VALUE_HEADS, query_group_count, HEAD_DIMENSION)
        scores = jnp.einsum('kgd,ptkd->pkgt', query_float, keys)
        scores = scores * (key_page_scale[page_ids][:, :, None, None] / math.sqrt(HEAD_DIMENSION))
        position = jnp.arange(MAXP, dtype=jnp.int32)[:, None] * PAGE_TOKENS + jnp.arange(PAGE_TOKENS, dtype=jnp.int32)[None, :]
        is_live = (position < length_row)[:, None, None, :]
        page_max = lax.optimization_barrier(jnp.max(jnp.where(is_live, scores, floor_score), axis=-1))
        weights = jnp.where(is_live, jnp.exp(scores - page_max[..., None]), 0.0)
        weights = lax.optimization_barrier(weights.astype(jnp.bfloat16)).astype(jnp.float32)
        page_sum = lax.optimization_barrier(jnp.sum(weights, axis=-1))
        page_out = jnp.einsum('pkgt,ptkd->pkgd', weights, value_rows) * value_page_scale[page_ids][:, :, None, None]
        peak = lax.optimization_barrier(jnp.max(page_max, axis=0))
        factor = jnp.exp(page_max - peak)
        numerator = lax.optimization_barrier(jnp.sum(page_out * factor[..., None], axis=0))
        denominator = lax.optimization_barrier(jnp.sum(page_sum * factor, axis=0))
        return (numerator / denominator[..., None]).reshape(QUERY_HEADS * HEAD_DIMENSION)
    attention = lax.map(per_request, (queries, lengths, page_table))
    return jnp.dot(attention.astype(jnp.bfloat16), out_weight, preferred_element_type=jnp.float32).astype(jnp.bfloat16)
```

```python
import functools
import math

import jax
import jax.numpy as jnp
from jax import lax
from jax.experimental import pallas as pl
from jax.experimental.pallas import tpu as pltpu
from jax.sharding import PartitionSpec as P

floor_score = float(jnp.bfloat16(-1e30))
LANES = 128
GROUP = 8
BLOCK = 256


def place_pages(gath_ref, offset, pages, width, tokens, placed_ref):
    requests = gath_ref.shape[0]
    page_rows = pages // LANES
    chunk = 16
    entry = lax.broadcasted_iota(jnp.int32, (chunk, LANES), 1).astype(jnp.float32)
    line = lax.broadcasted_iota(jnp.int32, (chunk, LANES), 0)
    sub = lax.broadcasted_iota(jnp.int32, (LANES, LANES), 0)
    sub_row = lax.broadcasted_iota(jnp.int32, (page_rows, LANES), 0)

    def step(c, total):
        rows = pl.ds(pl.multiple_of(c * chunk, chunk), chunk)
        high = gath_ref[rows, width : width + LANES].astype(jnp.float32)
        low = gath_ref[rows, width + LANES : width + 2 * LANES].astype(jnp.float32)
        lens = gath_ref[rows, width + 2 * LANES : width + 3 * LANES].astype(jnp.float32)
        length = lens[:, 0:1] * 256.0 + lens[:, 1:2]
        slot = (high * 256.0 + low).astype(jnp.int32) - offset
        inside = (slot >= 0) & (slot < pages)
        slot_row = jnp.where(inside, slot >> 7, -1)
        slot_lane = slot & (LANES - 1)
        live = jnp.clip(length - entry * float(tokens), 0.0, float(tokens))
        owner = c * chunk + line
        owner_high = (owner >> 7).astype(jnp.float32)
        owner_low = (owner & (LANES - 1)).astype(jnp.float32)
        lefts, rights = [], []
        for i in range(chunk):
            here = sub_row == slot_row[i : i + 1]
            parts = [
                jnp.where(here, v[i : i + 1], 0.0) for v in (owner_high, owner_low, live, live)
            ]
            lefts.append(jnp.concatenate(parts, axis=0).astype(jnp.bfloat16))
            rights.append(jnp.where(sub == slot_lane[i : i + 1], 1.0, 0.0).astype(jnp.bfloat16))
        return total + lax.dot_general(
            jnp.concatenate(lefts, axis=1),
            jnp.concatenate(rights, axis=1),
            (((1,), (1,)), ((), ())),
            preferred_element_type=jnp.float32,
        )

    start = jnp.zeros((4 * page_rows, LANES), jnp.float32)
    placed_ref[...] = lax.fori_loop(0, requests // chunk, step, start)


def attend_kernel(
    offset_ref,
    gath_ref,
    ks_ref,
    vs_ref,
    k_hbm,
    v_hbm,
    out_ref,
    k_buf,
    v_buf,
    placed_ref,
    cols_ref,
    owner_ref,
    qg_ref,
    po_ref,
    pm_ref,
    pmt_ref,
    acc_ref,
    m_ref,
    sems,
    *,
    heads,
    kv,
    tokens,
):
    requests = gath_ref.shape[0]
    width = heads * LANES
    pages = ks_ref.shape[1]
    blocks = pages // BLOCK
    page_rows = pages // LANES
    halves = BLOCK // LANES
    block_rows = BLOCK * tokens * kv
    group_rows = GROUP * tokens * kv
    per_kv = heads // kv

    def copies(b):
        rows = pl.ds(b * block_rows, block_rows)
        return (
            pltpu.make_async_copy(k_hbm.at[rows], k_buf.at[rows], sems.at[0, b]),
            pltpu.make_async_copy(v_hbm.at[rows], v_buf.at[rows], sems.at[1, b]),
        )

    for b in range(blocks):
        for copy in copies(b):
            copy.start()

    place_pages(gath_ref, offset_ref[0], pages, width, tokens, placed_ref)
    acc_ref[...] = jnp.zeros(acc_ref.shape, jnp.float32)
    m_ref[...] = jnp.full(m_ref.shape, floor_score, jnp.float32)

    col = lax.broadcasted_iota(jnp.int32, (GROUP, group_rows), 1)
    row = lax.broadcasted_iota(jnp.int32, (GROUP, group_rows), 0)
    token = (col % (tokens * kv)) // kv
    keys = [
        jnp.where((col // (tokens * kv) == row) & (col % kv == k), token, 2 * tokens).astype(
            jnp.float32
        )
        for k in range(kv)
    ]
    lane = lax.broadcasted_iota(jnp.int32, (GROUP, LANES), 1)
    sub8 = lax.broadcasted_iota(jnp.int32, (8, LANES), 0)
    lane_r = lax.broadcasted_iota(jnp.int32, (BLOCK, requests), 1).astype(jnp.float32)
    sub_r = lax.broadcasted_iota(jnp.int32, (requests, BLOCK), 0).astype(jnp.float32)
    ones = jnp.ones((group_rows, LANES), jnp.bfloat16)

    def block_step(b, carry):
        for u in range(halves):
            at = b * halves + u
            owner = placed_ref[pl.ds(at, 1), :] * 128.0 + placed_ref[pl.ds(page_rows + at, 1), :]
            live = placed_ref[pl.ds(2 * page_rows + at, 1), :]
            span = pl.ds(pl.multiple_of(at * LANES, LANES), LANES)
            rows = [owner, live]
            rows += [ks_ref[k : k + 1, span] * (1.0 / math.sqrt(LANES)) for k in range(kv)]
            rows += [vs_ref[k : k + 1, span] for k in range(kv)]
            stacked = jnp.zeros((8, LANES), jnp.float32)
            for i, r in enumerate(rows):
                stacked = jnp.where(sub8 == i, r, stacked)
            full = jnp.concatenate([stacked, jnp.zeros((LANES - 8, LANES), jnp.float32)], axis=0)
            cols_ref[u * LANES : (u + 1) * LANES, :] = full.T
            owner_ref[0:1, u * LANES : (u + 1) * LANES] = owner
        member_t = jnp.where(cols_ref[:, 0:1] == lane_r, 1.0, 0.0).astype(jnp.bfloat16)
        for h in range(0, heads, 2):
            pair = jnp.dot(
                member_t,
                gath_ref[:, h * LANES : (h + 2) * LANES],
                preferred_element_type=jnp.float32,
            )
            qg_ref[h] = pair[:, :LANES]
            qg_ref[h + 1] = pair[:, LANES:]
        for copy in copies(b):
            copy.wait()

        def group_step(g, inner):
            at = pl.ds(pl.multiple_of(g * GROUP, GROUP), GROUP)
            start = pl.multiple_of(b * block_rows + g * group_rows, group_rows)
            q = qg_ref[:, at, :].reshape(heads * GROUP, LANES).astype(jnp.bfloat16)
            s = lax.dot_general(
                q,
                k_buf[pl.ds(start, group_rows), :],
                (((1,), (1,)), ((), ())),
                preferred_element_type=jnp.float32,
            ).reshape(heads, GROUP, group_rows)
            c = cols_ref[at, :]
            peaks = jnp.zeros((GROUP, LANES), jnp.float32)
            probs = []
            for k in range(kv):
                live = keys[k] < c[:, 1:2]
                scale = c[:, 2 + k : 3 + k]
                for i in range(k * per_kv, (k + 1) * per_kv):
                    sk = jnp.where(live, s[i] * scale, floor_score)
                    mx = jnp.max(sk, axis=-1, keepdims=True)
                    probs.append(jnp.exp(sk - mx))
                    peaks = jnp.where(lane == i, mx, peaks)
            p = jnp.concatenate(probs, axis=0).astype(jnp.bfloat16)
            vg = jnp.concatenate([v_buf[pl.ds(start, group_rows), :], ones], axis=1)
            o = jnp.dot(p, vg, preferred_element_type=jnp.float32)
            o = o.reshape(heads, GROUP, 2 * LANES)
            for k in range(kv):
                hs = slice(k * per_kv, (k + 1) * per_kv)
                vscale = c[:, 2 + kv + k : 3 + kv + k]
                po_ref[hs, at, :LANES] = o[hs, :, :LANES] * vscale[None]
            po_ref[:, at, LANES:] = o[:, :, LANES:]
            pm_ref[at, :] = peaks
            return inner

        lax.fori_loop(0, BLOCK // GROUP, group_step, 0, unroll=4)
        for u in range(halves):
            span = slice(u * LANES, (u + 1) * LANES)
            pmt_ref[:, span] = pm_ref[span, :].T

        def head_step(h, inner):
            pm_row = pmt_ref[pl.ds(h, 1), :]
            member = sub_r == owner_ref[0:1, :]
            block_peak = jnp.max(
                jnp.where(member, pm_row, floor_score), axis=1, keepdims=True
            )
            old = m_ref[h]
            new = jnp.maximum(old, block_peak)
            alpha = jnp.exp(old - new)
            wide = jnp.concatenate([new] * halves, axis=1)
            w = jnp.exp(jnp.where(member, pm_row - wide, floor_score)).astype(jnp.bfloat16)
            o = jnp.dot(w, po_ref[h].astype(jnp.bfloat16), preferred_element_type=jnp.float32)
            acc_ref[h] = acc_ref[h] * jnp.concatenate([alpha, alpha], axis=1) + o
            m_ref[h] = new
            return inner

        lax.fori_loop(0, heads, head_step, 0, unroll=2)
        return carry

    lax.fori_loop(0, blocks, block_step, 0)

    lane_out = lax.broadcasted_iota(jnp.int32, (requests, LANES), 1)
    aux = jnp.zeros((requests, LANES), jnp.float32)
    for h in range(heads):
        peak = m_ref[h]
        shift = peak.astype(jnp.bfloat16).astype(jnp.float32)
        factor = jnp.exp(peak - shift)
        out_ref[:, h * LANES : (h + 1) * LANES] = (acc_ref[h, :, :LANES] * factor).astype(
            jnp.bfloat16
        )
        total = acc_ref[h, :, LANES:] * factor
        total_high = total.astype(jnp.bfloat16).astype(jnp.float32)
        aux = jnp.where(lane_out == h, shift, aux)
        aux = jnp.where(lane_out == heads + h, total_high, aux)
        aux = jnp.where(lane_out == 2 * heads + h, total - total_high, aux)
    out_ref[:, width : width + LANES] = aux.astype(jnp.bfloat16)


def attend(gathered, offset, k_rows, v_rows, ks, vs, heads, kv, tokens):
    requests = gathered.shape[0]
    pages = ks.shape[1]
    f32 = jnp.float32
    vmem = pl.BlockSpec(memory_space=pltpu.VMEM)
    hbm = pl.BlockSpec(memory_space=pl.ANY)
    return pl.pallas_call(
        functools.partial(attend_kernel, heads=heads, kv=kv, tokens=tokens),
        out_shape=jax.ShapeDtypeStruct((requests, (heads + 1) * LANES), jnp.bfloat16),
        in_specs=[pl.BlockSpec(memory_space=pltpu.SMEM), vmem, vmem, vmem, hbm, hbm],
        out_specs=vmem,
        scratch_shapes=[
            pltpu.VMEM(k_rows.shape, k_rows.dtype),
            pltpu.VMEM(v_rows.shape, v_rows.dtype),
            pltpu.VMEM((4 * (pages // LANES), LANES), f32),
            pltpu.VMEM((BLOCK, LANES), f32),
            pltpu.VMEM((8, BLOCK), f32),
            pltpu.VMEM((heads, BLOCK, LANES), f32),
            pltpu.VMEM((heads, BLOCK, 2 * LANES), f32),
            pltpu.VMEM((BLOCK, LANES), f32),
            pltpu.VMEM((LANES, BLOCK), f32),
            pltpu.VMEM((heads, requests, 2 * LANES), f32),
            pltpu.VMEM((heads, requests, LANES), f32),
            pltpu.SemaphoreType.DMA((2, pages // BLOCK)),
        ],
        compiler_params=pltpu.CompilerParams(vmem_limit_bytes=60 * 1024 * 1024),
        name="attend",
    )(offset, gathered, ks, vs, k_rows, v_rows)


def combine_kernel(in_ref, out_ref, *, heads):
    sources = in_ref.shape[0]
    width = heads * LANES
    aux = in_ref[:, :, width:].astype(jnp.float32)
    shift = aux[:, :, :heads]
    total = aux[:, :, heads : 2 * heads] + aux[:, :, 2 * heads : 3 * heads]
    factor = jnp.exp(shift - jnp.max(shift, axis=0, keepdims=True))
    factor = factor / jnp.sum(total * factor, axis=0, keepdims=True)
    for h in range(heads):
        span = slice(h * LANES, (h + 1) * LANES)
        value = in_ref[0, :, span].astype(jnp.float32) * factor[0, :, h : h + 1]
        for s in range(1, sources):
            value += in_ref[s, :, span].astype(jnp.float32) * factor[s, :, h : h + 1]
        out_ref[:, span] = value.astype(jnp.bfloat16)


def combine(parts, heads):
    rows = parts.shape[1]
    return pl.pallas_call(
        functools.partial(combine_kernel, heads=heads),
        out_shape=jax.ShapeDtypeStruct((rows, heads * LANES), jnp.bfloat16),
        name="combine",
    )(parts)


def project_kernel(x_ref, w_ref, out_ref):
    out_ref[0] = jnp.dot(x_ref[...], w_ref[...], preferred_element_type=jnp.float32).astype(
        jnp.bfloat16
    )


def project(x, weight, pieces):
    rows, depth = x.shape
    columns = weight.shape[1]
    piece = columns // pieces
    if piece % LANES:
        terms = jnp.dot(x, weight, preferred_element_type=jnp.float32).astype(jnp.bfloat16)
        return terms.reshape(rows, pieces, piece).transpose(1, 0, 2)
    return pl.pallas_call(
        project_kernel,
        grid=(pieces,),
        out_shape=jax.ShapeDtypeStruct((pieces, rows, piece), jnp.bfloat16),
        in_specs=[
            pl.BlockSpec((rows, depth), lambda i: (0, 0)),
            pl.BlockSpec((depth, piece), lambda i: (0, i)),
        ],
        out_specs=pl.BlockSpec((1, rows, piece), lambda i: (i, 0, 0)),
        name="project",
    )(x, weight)


def spread(x, axis):
    count = lax.axis_size(axis)
    copies = jnp.broadcast_to(x[None], (count,) + x.shape)
    out = lax.all_to_all(copies, axis, split_axis=0, concat_axis=0, tiled=True)
    return out.reshape((count * x.shape[0],) + x.shape[1:])


def pack_request(queries, lengths, page_table):
    rows, heads, head_size = queries.shape
    high = page_table >> 8
    low = page_table & 255
    pair = jnp.stack([lengths >> 8, lengths & 255], axis=1)
    pad = [
        jnp.pad(part.astype(jnp.bfloat16), ((0, 0), (0, LANES - part.shape[1])))
        for part in (high, low, pair)
    ]
    return jnp.concatenate([queries.reshape(rows, heads * head_size)] + pad, axis=1)


def on_device(
    queries,
    k_codes,
    value_quantized_codes,
    key_page_scale,
    value_page_scale,
    lengths,
    page_table,
    out_weight,
):
    pages, tokens, kv, head_size = k_codes.shape
    rows, heads, _ = queries.shape
    gathered = spread(pack_request(queries, lengths, page_table), "req")
    offset = (lax.axis_index("req") * pages).astype(jnp.int32).reshape(1)
    partial = attend(
        gathered,
        offset,
        k_codes.reshape(pages * tokens * kv, head_size),
        value_quantized_codes.reshape(pages * tokens * kv, head_size),
        key_page_scale.T,
        value_page_scale.T,
        heads,
        kv,
        tokens,
    )
    sources = lax.axis_size("req")
    parts = lax.all_to_all(
        partial.reshape(sources, rows, partial.shape[1]),
        "req",
        split_axis=0,
        concat_axis=0,
        tiled=True,
    )
    attention = spread(combine(parts, heads), "req")
    terms = project(attention, out_weight, lax.axis_size("head"))
    terms = lax.all_to_all(terms, "head", split_axis=0, concat_axis=0, tiled=True)
    return jnp.sum(terms.astype(jnp.float32), axis=0).astype(jnp.bfloat16)


def solution(mesh):
    in_specs = (
        P("req", "head", None),
        P("req", None, "head", None),
        P("req", None, "head", None),
        P("req", "head"),
        P("req", "head"),
        P("req"),
        P("req", None),
        P("head", "req"),
    )
    out_specs = P(None, ("req", "head"))
    return jax.shard_map(
        on_device, mesh=mesh, in_specs=in_specs, out_specs=out_specs, check_vma=False
    )
```

```python
import functools
import math

import jax
import jax.numpy as jnp
from jax import lax
from jax.experimental import pallas as pl
from jax.experimental.pallas import tpu as pltpu
from jax.sharding import PartitionSpec as P

floor_score = float(jnp.bfloat16(-1e30))
LANES = 128
GROUP = 8
BLOCK = 256


def place_pages(gath_ref, offset, pages, width, placed_ref):
    requests = gath_ref.shape[0]
    page_rows = pages // LANES
    chunk = 16
    line = lax.broadcasted_iota(jnp.int32, (chunk, LANES), 0)
    sub = lax.broadcasted_iota(jnp.int32, (LANES, LANES), 0)
    sub_row = lax.broadcasted_iota(jnp.int32, (page_rows, LANES), 0)

    def step(c, total):
        rows = pl.ds(pl.multiple_of(c * chunk, chunk), chunk)
        high = gath_ref[rows, width : width + LANES].astype(jnp.float32)
        low = gath_ref[rows, width + LANES : width + 2 * LANES].astype(jnp.float32)
        live = gath_ref[rows, width + 2 * LANES : width + 3 * LANES].astype(jnp.float32)
        slot = (high * 256.0 + low).astype(jnp.int32) - offset
        inside = (slot >= 0) & (slot < pages)
        slot_row = jnp.where(inside, slot >> 7, -1)
        slot_lane = slot & (LANES - 1)
        owner = c * chunk + line
        owner_high = (owner >> 7).astype(jnp.float32)
        owner_low = (owner & (LANES - 1)).astype(jnp.float32)
        lefts, rights = [], []
        for i in range(chunk):
            here = sub_row == slot_row[i : i + 1]
            parts = [
                jnp.where(here, v[i : i + 1], 0.0) for v in (owner_high, owner_low, live, live)
            ]
            lefts.append(jnp.concatenate(parts, axis=0).astype(jnp.bfloat16))
            rights.append(jnp.where(sub == slot_lane[i : i + 1], 1.0, 0.0).astype(jnp.bfloat16))
        return total + lax.dot_general(
            jnp.concatenate(lefts, axis=1),
            jnp.concatenate(rights, axis=1),
            (((1,), (1,)), ((), ())),
            preferred_element_type=jnp.float32,
        )

    start = jnp.zeros((4 * page_rows, LANES), jnp.float32)
    placed_ref[...] = lax.fori_loop(0, requests // chunk, step, start)


def attend_kernel(
    index_ref,
    gath_ref,
    ks_ref,
    vs_ref,
    k_hbm,
    v_hbm,
    *rest,
    heads,
    kv,
    tokens,
    sources,
):
    out_refs, scratch = rest[:sources], rest[sources:]
    (
        k_buf,
        v_buf,
        placed_ref,
        cols_ref,
        owner_ref,
        qg_ref,
        po_ref,
        pm_ref,
        pmt_ref,
        acc_ref,
        m_ref,
        sems,
    ) = scratch
    requests = gath_ref.shape[0]
    width = heads * LANES
    pages = ks_ref.shape[1]
    blocks = pages // BLOCK
    page_rows = pages // LANES
    halves = BLOCK // LANES
    block_rows = BLOCK * tokens * kv
    group_rows = GROUP * tokens * kv
    per_kv = heads // kv

    def copies(b):
        rows = pl.ds(b * block_rows, block_rows)
        return (
            pltpu.make_async_copy(k_hbm.at[rows], k_buf.at[rows], sems.at[0, b]),
            pltpu.make_async_copy(v_hbm.at[rows], v_buf.at[rows], sems.at[1, b]),
        )

    for b in range(blocks):
        for copy in copies(b):
            copy.start()

    place_pages(gath_ref, index_ref[0] * pages, pages, width, placed_ref)
    acc_ref[...] = jnp.zeros(acc_ref.shape, jnp.float32)
    m_ref[...] = jnp.full(m_ref.shape, floor_score, jnp.float32)

    col = lax.broadcasted_iota(jnp.int32, (GROUP, group_rows), 1)
    row = lax.broadcasted_iota(jnp.int32, (GROUP, group_rows), 0)
    token = (col % (tokens * kv)) // kv
    keys = [
        jnp.where((col // (tokens * kv) == row) & (col % kv == k), token, 2 * tokens).astype(
            jnp.float32
        )
        for k in range(kv)
    ]
    lane = lax.broadcasted_iota(jnp.int32, (GROUP, LANES), 1)
    sub8 = lax.broadcasted_iota(jnp.int32, (8, LANES), 0)
    lane_r = lax.broadcasted_iota(jnp.int32, (BLOCK, requests), 1).astype(jnp.float32)
    sub_r = lax.broadcasted_iota(jnp.int32, (requests, BLOCK), 0).astype(jnp.float32)
    ones = jnp.ones((group_rows, LANES), jnp.bfloat16)

    def block_step(b, carry):
        for u in range(halves):
            at = b * halves + u
            owner = placed_ref[pl.ds(at, 1), :] * 128.0 + placed_ref[pl.ds(page_rows + at, 1), :]
            live = placed_ref[pl.ds(2 * page_rows + at, 1), :]
            span = pl.ds(pl.multiple_of(at * LANES, LANES), LANES)
            rows = [owner, live]
            rows += [ks_ref[k : k + 1, span] * (1.0 / math.sqrt(LANES)) for k in range(kv)]
            rows += [vs_ref[k : k + 1, span] for k in range(kv)]
            stacked = jnp.zeros((8, LANES), jnp.float32)
            for i, r in enumerate(rows):
                stacked = jnp.where(sub8 == i, r, stacked)
            full = jnp.concatenate([stacked, jnp.zeros((LANES - 8, LANES), jnp.float32)], axis=0)
            cols_ref[u * LANES : (u + 1) * LANES, :] = full.T
            owner_ref[0:1, u * LANES : (u + 1) * LANES] = owner
        member_t = jnp.where(cols_ref[:, 0:1] == lane_r, 1.0, 0.0).astype(jnp.bfloat16)
        for h in range(0, heads, 2):
            pair = jnp.dot(
                member_t,
                gath_ref[:, h * LANES : (h + 2) * LANES],
                preferred_element_type=jnp.float32,
            )
            qg_ref[h] = pair[:, :LANES]
            qg_ref[h + 1] = pair[:, LANES:]
        for copy in copies(b):
            copy.wait()

        def group_step(g, inner):
            at = pl.ds(pl.multiple_of(g * GROUP, GROUP), GROUP)
            start = pl.multiple_of(b * block_rows + g * group_rows, group_rows)
            q = qg_ref[:, at, :].reshape(heads * GROUP, LANES).astype(jnp.bfloat16)
            s = lax.dot_general(
                q,
                k_buf[pl.ds(start, group_rows), :],
                (((1,), (1,)), ((), ())),
                preferred_element_type=jnp.float32,
            ).reshape(heads, GROUP, group_rows)
            c = cols_ref[at, :]
            peaks = jnp.zeros((GROUP, LANES), jnp.float32)
            probs = []
            for k in range(kv):
                live = keys[k] < c[:, 1:2]
                scale = c[:, 2 + k : 3 + k]
                for i in range(k * per_kv, (k + 1) * per_kv):
                    sk = jnp.where(live, s[i] * scale, floor_score)
                    mx = jnp.max(sk, axis=-1, keepdims=True)
                    probs.append(jnp.exp(sk - mx))
                    peaks = jnp.where(lane == i, mx, peaks)
            p = jnp.concatenate(probs, axis=0).astype(jnp.bfloat16)
            vg = jnp.concatenate([v_buf[pl.ds(start, group_rows), :], ones], axis=1)
            o = jnp.dot(p, vg, preferred_element_type=jnp.float32)
            o = o.reshape(heads, GROUP, 2 * LANES)
            for k in range(kv):
                hs = slice(k * per_kv, (k + 1) * per_kv)
                vscale = c[:, 2 + kv + k : 3 + kv + k]
                po_ref[hs, at, :LANES] = o[hs, :, :LANES] * vscale[None]
            po_ref[:, at, LANES:] = o[:, :, LANES:]
            pm_ref[at, :] = peaks
            return inner

        lax.fori_loop(0, BLOCK // GROUP, group_step, 0, unroll=4)
        for u in range(halves):
            span = slice(u * LANES, (u + 1) * LANES)
            pmt_ref[:, span] = pm_ref[span, :].T

        def head_step(h, inner):
            pm_row = pmt_ref[pl.ds(h, 1), :]
            member = sub_r == owner_ref[0:1, :]
            block_peak = jnp.max(
                jnp.where(member, pm_row, floor_score), axis=1, keepdims=True
            )
            old = m_ref[h]
            new = jnp.maximum(old, block_peak)
            alpha = jnp.exp(old - new)
            wide = jnp.concatenate([new] * halves, axis=1)
            w = jnp.exp(jnp.where(member, pm_row - wide, floor_score)).astype(jnp.bfloat16)
            o = jnp.dot(w, po_ref[h].astype(jnp.bfloat16), preferred_element_type=jnp.float32)
            acc_ref[h] = acc_ref[h] * jnp.concatenate([alpha, alpha], axis=1) + o
            m_ref[h] = new
            return inner

        lax.fori_loop(0, heads, head_step, 0, unroll=2)
        return carry

    lax.fori_loop(0, blocks, block_step, 0)

    rows = requests // sources
    lane_out = lax.broadcasted_iota(jnp.int32, (rows, LANES), 1)
    for d in range(sources):
        target = lax.rem(index_ref[0] + d, sources)
        here = pl.ds(pl.multiple_of(target * rows, rows), rows)
        aux = jnp.zeros((rows, LANES), jnp.float32)
        for h in range(heads):
            peak = m_ref[h, here, :]
            shift = peak.astype(jnp.bfloat16).astype(jnp.float32)
            factor = jnp.exp(peak - shift)
            out_refs[d][:, h * LANES : (h + 1) * LANES] = (
                acc_ref[h, here, :LANES] * factor
            ).astype(jnp.bfloat16)
            total = acc_ref[h, here, LANES:] * factor
            total_high = total.astype(jnp.bfloat16).astype(jnp.float32)
            aux = jnp.where(lane_out == h, shift, aux)
            aux = jnp.where(lane_out == heads + h, total_high, aux)
            aux = jnp.where(lane_out == 2 * heads + h, total - total_high, aux)
        out_refs[d][:, width : width + LANES] = aux.astype(jnp.bfloat16)


def attend(gathered, index, k_rows, v_rows, ks, vs, heads, kv, tokens, sources):
    requests = gathered.shape[0]
    pages = ks.shape[1]
    f32 = jnp.float32
    vmem = pl.BlockSpec(memory_space=pltpu.VMEM)
    hbm = pl.BlockSpec(memory_space=pl.ANY)
    return pl.pallas_call(
        functools.partial(attend_kernel, heads=heads, kv=kv, tokens=tokens, sources=sources),
        out_shape=[
            jax.ShapeDtypeStruct((requests // sources, (heads + 1) * LANES), jnp.bfloat16)
        ]
        * sources,
        in_specs=[pl.BlockSpec(memory_space=pltpu.SMEM), vmem, vmem, vmem, hbm, hbm],
        out_specs=[vmem] * sources,
        scratch_shapes=[
            pltpu.VMEM(k_rows.shape, k_rows.dtype),
            pltpu.VMEM(v_rows.shape, v_rows.dtype),
            pltpu.VMEM((4 * (pages // LANES), LANES), f32),
            pltpu.VMEM((BLOCK, LANES), f32),
            pltpu.VMEM((8, BLOCK), f32),
            pltpu.VMEM((heads, BLOCK, LANES), f32),
            pltpu.VMEM((heads, BLOCK, 2 * LANES), f32),
            pltpu.VMEM((BLOCK, LANES), f32),
            pltpu.VMEM((LANES, BLOCK), f32),
            pltpu.VMEM((heads, requests, 2 * LANES), f32),
            pltpu.VMEM((heads, requests, LANES), f32),
            pltpu.SemaphoreType.DMA((2, pages // BLOCK)),
        ],
        compiler_params=pltpu.CompilerParams(vmem_limit_bytes=60 * 1024 * 1024),
        name="attend",
    )(index, gathered, ks, vs, k_rows, v_rows)


def combine_kernel(*refs, heads):
    in_refs, out_ref = refs[:-1], refs[-1]
    width = heads * LANES
    aux = [ref[:, width:].astype(jnp.float32) for ref in in_refs]
    shift = [a[:, :heads] for a in aux]
    total = [a[:, heads : 2 * heads] + a[:, 2 * heads : 3 * heads] for a in aux]
    overall = functools.reduce(jnp.maximum, shift)
    factor = [jnp.exp(a - overall) for a in shift]
    whole = sum(t * f for t, f in zip(total, factor))
    factor = [f / whole for f in factor]
    for h in range(heads):
        span = slice(h * LANES, (h + 1) * LANES)
        value = sum(
            ref[:, span].astype(jnp.float32) * f[:, h : h + 1] for ref, f in zip(in_refs, factor)
        )
        out_ref[:, span] = value.astype(jnp.bfloat16)


def combine(parts, heads):
    return pl.pallas_call(
        functools.partial(combine_kernel, heads=heads),
        out_shape=jax.ShapeDtypeStruct((parts[0].shape[0], heads * LANES), jnp.bfloat16),
        name="combine",
    )(*parts)


def project_kernel(index_ref, x_ref, w_hbm, *rest):
    out_refs, (w_buf, sems) = rest[:-2], rest[-2:]
    pieces, _, piece = w_buf.shape
    copies = []
    for d in range(pieces):
        at = pl.multiple_of(lax.rem(index_ref[0] + d, pieces) * piece, piece)
        copies.append(
            pltpu.make_async_copy(w_hbm.at[:, pl.ds(at, piece)], w_buf.at[d], sems.at[d])
        )
    for copy in copies:
        copy.start()
    for d in range(pieces):
        copies[d].wait()
        out_refs[d][...] = jnp.dot(
            x_ref[...], w_buf[d], preferred_element_type=jnp.float32
        ).astype(jnp.bfloat16)


def project(x, weight, index, pieces):
    rows, depth = x.shape
    columns = weight.shape[1]
    piece = columns // pieces
    if piece % LANES:
        terms = jnp.dot(x, weight, preferred_element_type=jnp.float32).astype(jnp.bfloat16)
        return [
            lax.dynamic_slice_in_dim(terms, ((index[0] + d) % pieces) * piece, piece, 1)
            for d in range(pieces)
        ]
    vmem = pl.BlockSpec(memory_space=pltpu.VMEM)
    return pl.pallas_call(
        project_kernel,
        out_shape=[jax.ShapeDtypeStruct((rows, piece), jnp.bfloat16)] * pieces,
        in_specs=[
            pl.BlockSpec(memory_space=pltpu.SMEM),
            vmem,
            pl.BlockSpec(memory_space=pl.ANY),
        ],
        out_specs=[vmem] * pieces,
        scratch_shapes=[
            pltpu.VMEM((pieces, depth, piece), weight.dtype),
            pltpu.SemaphoreType.DMA((pieces,)),
        ],
        name="project",
    )(index, x, weight)


def exchange(parts, axis):
    count = len(parts)
    return [parts[0]] + [
        lax.ppermute(parts[d], axis, [(s, (s + d) % count) for s in range(count)])
        for d in range(1, count)
    ]


def pack_kernel(q_ref, len_ref, table_ref, out_ref, *, tokens):
    rows, heads, _ = q_ref.shape
    width = heads * LANES
    queries = jnp.transpose(q_ref[...].astype(jnp.float32), (1, 0, 2))
    for h in range(heads):
        out_ref[:, h * LANES : (h + 1) * LANES] = queries[h].astype(jnp.bfloat16)
    table = table_ref[...]
    out_ref[:, width : width + LANES] = (table >> 8).astype(jnp.float32).astype(jnp.bfloat16)
    out_ref[:, width + LANES : width + 2 * LANES] = (
        (table & 255).astype(jnp.float32).astype(jnp.bfloat16)
    )
    diagonal = lax.broadcasted_iota(jnp.int32, (rows, rows), 0) == lax.broadcasted_iota(
        jnp.int32, (rows, rows), 1
    )
    lengths = len_ref[...].astype(jnp.float32)
    length = jnp.sum(jnp.where(diagonal, lengths, 0.0), axis=1, keepdims=True)
    entry = lax.broadcasted_iota(jnp.int32, table.shape, 1).astype(jnp.float32)
    live = jnp.clip(length - entry * float(tokens), 0.0, float(tokens))
    out_ref[:, width + 2 * LANES :] = live.astype(jnp.bfloat16)


def pack_request(queries, lengths, page_table, tokens):
    rows, heads, _ = queries.shape
    page_table = jnp.pad(
        page_table, ((0, 0), (0, LANES - page_table.shape[1])), constant_values=-1
    )
    return pl.pallas_call(
        functools.partial(pack_kernel, tokens=tokens),
        out_shape=jax.ShapeDtypeStruct((rows, (heads + 3) * LANES), jnp.bfloat16),
        name="pack",
    )(queries, lengths.reshape(1, rows), page_table)


def on_device(
    queries,
    k_codes,
    value_quantized_codes,
    key_page_scale,
    value_page_scale,
    lengths,
    page_table,
    out_weight,
):
    pages, tokens, kv, head_size = k_codes.shape
    rows, heads, _ = queries.shape
    sources = lax.axis_size("req")
    request = pack_request(queries, lengths, page_table, tokens)
    gathered = lax.all_gather(request, "req", axis=0, tiled=True)
    partial = attend(
        gathered,
        lax.axis_index("req").astype(jnp.int32).reshape(1),
        k_codes.reshape(pages * tokens * kv, head_size),
        value_quantized_codes.reshape(pages * tokens * kv, head_size),
        key_page_scale.T,
        value_page_scale.T,
        heads,
        kv,
        tokens,
        sources,
    )
    attention = combine(exchange(partial, "req"), heads)
    attention = lax.all_gather(attention, "req", axis=0, tiled=True)
    index = lax.axis_index("head").astype(jnp.int32).reshape(1)
    terms = exchange(project(attention, out_weight, index, lax.axis_size("head")), "head")
    return sum(t.astype(jnp.float32) for t in terms).astype(jnp.bfloat16)


def solution(mesh):
    in_specs = (
        P("req", "head", None),
        P("req", None, "head", None),
        P("req", None, "head", None),
        P("req", "head"),
        P("req", "head"),
        P("req"),
        P("req", None),
        P("head", "req"),
    )
    out_specs = P(None, ("req", "head"))
    return jax.shard_map(
        on_device, mesh=mesh, in_specs=in_specs, out_specs=out_specs, check_vma=False
    )
```

```python
import functools
import math

import jax
import jax.numpy as jnp
from jax import lax
from jax.experimental import pallas as pl
from jax.experimental.pallas import tpu as pltpu
from jax.sharding import PartitionSpec as P

floor_score = float(jnp.bfloat16(-1e30))
LANES = 128
GROUP = 8
BLOCK = 256


def place_pages(gath_ref, offset, pages, width, placed_ref):
    requests = gath_ref.shape[0]
    page_rows = pages // LANES
    chunk = 16
    line = lax.broadcasted_iota(jnp.int32, (chunk, LANES), 0)
    sub = lax.broadcasted_iota(jnp.int32, (LANES, LANES), 0)
    sub_row = lax.broadcasted_iota(jnp.int32, (page_rows, LANES), 0)

    def step(c, total):
        rows = pl.ds(pl.multiple_of(c * chunk, chunk), chunk)
        high = gath_ref[rows, width : width + LANES].astype(jnp.float32)
        low = gath_ref[rows, width + LANES : width + 2 * LANES].astype(jnp.float32)
        live = gath_ref[rows, width + 2 * LANES : width + 3 * LANES].astype(jnp.float32)
        slot = (high * 256.0 + low).astype(jnp.int32) - offset
        inside = (slot >= 0) & (slot < pages)
        slot_row = jnp.where(inside, slot >> 7, -1)
        slot_lane = slot & (LANES - 1)
        owner = c * chunk + line
        owner_high = (owner >> 7).astype(jnp.float32)
        owner_low = (owner & (LANES - 1)).astype(jnp.float32)
        for first in range(0, chunk, 2):
            lefts, rights = [], []
            for i in (first, first + 1):
                here = sub_row == slot_row[i : i + 1]
                parts = [
                    jnp.where(here, v[i : i + 1], 0.0) for v in (owner_high, owner_low, live, live)
                ]
                lefts.append(jnp.concatenate(parts, axis=0).astype(jnp.bfloat16))
                rights.append(
                    jnp.where(sub == slot_lane[i : i + 1], 1.0, 0.0).astype(jnp.bfloat16)
                )
            total += lax.dot_general(
                jnp.concatenate(lefts, axis=1),
                jnp.concatenate(rights, axis=1),
                (((1,), (1,)), ((), ())),
                preferred_element_type=jnp.float32,
            )
        return total

    start = jnp.zeros((4 * page_rows, LANES), jnp.float32)
    placed_ref[...] = lax.fori_loop(0, requests // chunk, step, start)


def attend_kernel(
    index_ref,
    gath_ref,
    ks_ref,
    vs_ref,
    k_hbm,
    v_hbm,
    w_hbm,
    *rest,
    heads,
    kv,
    tokens,
    sources,
):
    out_refs, w_out, scratch = rest[:sources], rest[sources], rest[sources + 1 :]
    (
        k_buf,
        v_buf,
        placed_ref,
        cols_ref,
        owner_ref,
        qg_ref,
        po_ref,
        pm_ref,
        pmt_ref,
        acc_ref,
        m_ref,
        sems,
        w_sems,
    ) = scratch
    requests = gath_ref.shape[0]
    width = heads * LANES
    pages = ks_ref.shape[1]
    blocks = pages // BLOCK
    page_rows = pages // LANES
    halves = BLOCK // LANES
    block_rows = BLOCK * tokens * kv
    group_rows = GROUP * tokens * kv
    per_kv = heads // kv

    def copies(b):
        rows = pl.ds(b * block_rows, block_rows)
        return (
            pltpu.make_async_copy(k_hbm.at[rows], k_buf.at[rows], sems.at[0, b]),
            pltpu.make_async_copy(v_hbm.at[rows], v_buf.at[rows], sems.at[1, b]),
        )

    pieces, _, piece = w_out.shape
    w_copies = []
    for d in range(pieces):
        at = pl.multiple_of(lax.rem(index_ref[1] + d, pieces) * piece, piece)
        w_copies.append(
            pltpu.make_async_copy(w_hbm.at[:, pl.ds(at, piece)], w_out.at[d], w_sems.at[d])
        )
    for b in range(blocks):
        for copy in copies(b):
            copy.start()
    for copy in w_copies:
        copy.start()

    place_pages(gath_ref, index_ref[0] * pages, pages, width, placed_ref)
    acc_ref[...] = jnp.zeros(acc_ref.shape, jnp.float32)
    m_ref[...] = jnp.full(m_ref.shape, floor_score, jnp.float32)

    col = lax.broadcasted_iota(jnp.int32, (GROUP, group_rows), 1)
    row = lax.broadcasted_iota(jnp.int32, (GROUP, group_rows), 0)
    token = (col % (tokens * kv)) // kv
    keys = [
        jnp.where((col // (tokens * kv) == row) & (col % kv == k), token, 2 * tokens).astype(
            jnp.float32
        )
        for k in range(kv)
    ]
    lane = lax.broadcasted_iota(jnp.int32, (GROUP, LANES), 1)
    sub8 = lax.broadcasted_iota(jnp.int32, (8, LANES), 0)
    lane_r = lax.broadcasted_iota(jnp.int32, (BLOCK, requests), 1).astype(jnp.float32)
    sub_r = lax.broadcasted_iota(jnp.int32, (requests, BLOCK), 0).astype(jnp.float32)
    ones = jnp.ones((group_rows, LANES), jnp.bfloat16)

    def block_step(b, carry):
        for u in range(halves):
            at = b * halves + u
            owner = placed_ref[pl.ds(at, 1), :] * 128.0 + placed_ref[pl.ds(page_rows + at, 1), :]
            live = placed_ref[pl.ds(2 * page_rows + at, 1), :]
            span = pl.ds(pl.multiple_of(at * LANES, LANES), LANES)
            rows = [owner, live]
            rows += [ks_ref[k : k + 1, span] * (math.log2(math.e) / math.sqrt(LANES)) for k in range(kv)]
            rows += [vs_ref[k : k + 1, span] for k in range(kv)]
            stacked = jnp.zeros((8, LANES), jnp.float32)
            for i, r in enumerate(rows):
                stacked = jnp.where(sub8 == i, r, stacked)
            full = jnp.concatenate([stacked, jnp.zeros((LANES - 8, LANES), jnp.float32)], axis=0)
            cols_ref[u * LANES : (u + 1) * LANES, :] = full.T
            owner_ref[0:1, u * LANES : (u + 1) * LANES] = owner
        member_t = jnp.where(cols_ref[:, 0:1] == lane_r, 1.0, 0.0).astype(jnp.bfloat16)
        for h in range(0, heads, 2):
            pair = jnp.dot(
                member_t,
                gath_ref[:, h * LANES : (h + 2) * LANES],
                preferred_element_type=jnp.float32,
            )
            qg_ref[h] = pair[:, :LANES]
            qg_ref[h + 1] = pair[:, LANES:]
        for copy in copies(b):
            copy.wait()

        def group_step(g, inner):
            at = pl.ds(pl.multiple_of(g * GROUP, GROUP), GROUP)
            start = pl.multiple_of(b * block_rows + g * group_rows, group_rows)
            q = qg_ref[:, at, :].reshape(heads * GROUP, LANES).astype(jnp.bfloat16)
            s = lax.dot_general(
                q,
                k_buf[pl.ds(start, group_rows), :],
                (((1,), (1,)), ((), ())),
                preferred_element_type=jnp.float32,
            ).reshape(heads, GROUP, group_rows)
            c = cols_ref[at, :]
            peaks = jnp.zeros((GROUP, LANES), jnp.float32)
            probs = []
            for k in range(kv):
                live = keys[k] < c[:, 1:2]
                scale = c[:, 2 + k : 3 + k]
                for i in range(k * per_kv, (k + 1) * per_kv):
                    sk = jnp.where(live, s[i] * scale, floor_score)
                    mx = jnp.max(sk, axis=-1, keepdims=True)
                    probs.append(jnp.exp2(sk - mx))
                    peaks = jnp.where(lane == i, mx, peaks)
            p = jnp.concatenate(probs, axis=0).astype(jnp.bfloat16)
            vg = jnp.concatenate([v_buf[pl.ds(start, group_rows), :], ones], axis=1)
            o = jnp.dot(p, vg, preferred_element_type=jnp.float32)
            o = o.reshape(heads, GROUP, 2 * LANES)
            for k in range(kv):
                hs = slice(k * per_kv, (k + 1) * per_kv)
                vscale = c[:, 2 + kv + k : 3 + kv + k]
                po_ref[hs, at, :LANES] = o[hs, :, :LANES] * vscale[None]
            po_ref[:, at, LANES:] = o[:, :, LANES:]
            pm_ref[at, :] = peaks
            return inner

        lax.fori_loop(0, BLOCK // GROUP, group_step, 0, unroll=8)
        for u in range(halves):
            span = slice(u * LANES, (u + 1) * LANES)
            pmt_ref[:, span] = pm_ref[span, :].T

        def head_step(h, inner):
            pm_row = pmt_ref[pl.ds(h, 1), :]
            member = sub_r == owner_ref[0:1, :]
            block_peak = jnp.max(
                jnp.where(member, pm_row, floor_score), axis=1, keepdims=True
            )
            old = m_ref[h]
            new = jnp.maximum(old, block_peak)
            alpha = jnp.exp2(old - new)
            wide = jnp.concatenate([new] * halves, axis=1)
            w = jnp.exp2(jnp.where(member, pm_row - wide, floor_score)).astype(jnp.bfloat16)
            o = jnp.dot(w, po_ref[h].astype(jnp.bfloat16), preferred_element_type=jnp.float32)
            acc_ref[h] = acc_ref[h] * jnp.concatenate([alpha, alpha], axis=1) + o
            m_ref[h] = new
            return inner

        lax.fori_loop(0, heads, head_step, 0, unroll=4)
        return carry

    lax.fori_loop(0, blocks, block_step, 0)

    rows = requests // sources
    lane_out = lax.broadcasted_iota(jnp.int32, (rows, LANES), 1)
    for d in range(sources):
        target = lax.rem(index_ref[0] + d, sources)
        here = pl.ds(pl.multiple_of(target * rows, rows), rows)
        aux = jnp.zeros((rows, LANES), jnp.float32)
        for h in range(heads):
            peak = m_ref[h, here, :]
            shift = peak.astype(jnp.bfloat16).astype(jnp.float32)
            factor = jnp.exp2(peak - shift)
            out_refs[d][:, h * LANES : (h + 1) * LANES] = (
                acc_ref[h, here, :LANES] * factor
            ).astype(jnp.bfloat16)
            total = acc_ref[h, here, LANES:] * factor
            total_high = total.astype(jnp.bfloat16).astype(jnp.float32)
            aux = jnp.where(lane_out == h, shift, aux)
            aux = jnp.where(lane_out == heads + h, total_high, aux)
            aux = jnp.where(lane_out == 2 * heads + h, total - total_high, aux)
        out_refs[d][:, width : width + LANES] = aux.astype(jnp.bfloat16)
    for copy in w_copies:
        copy.wait()


def attend(gathered, index, k_rows, v_rows, ks, vs, weight, pieces, heads, kv, tokens, sources):
    depth, columns = weight.shape
    requests = gathered.shape[0]
    pages = ks.shape[1]
    f32 = jnp.float32
    vmem = pl.BlockSpec(memory_space=pltpu.VMEM)
    hbm = pl.BlockSpec(memory_space=pl.ANY)
    return pl.pallas_call(
        functools.partial(attend_kernel, heads=heads, kv=kv, tokens=tokens, sources=sources),
        out_shape=[
            jax.ShapeDtypeStruct((requests // sources, (heads + 1) * LANES), jnp.bfloat16)
        ]
        * sources
        + [pltpu.VMEM((pieces, depth, columns // pieces), weight.dtype)],
        in_specs=[pl.BlockSpec(memory_space=pltpu.SMEM), vmem, vmem, vmem, hbm, hbm, hbm],
        out_specs=[vmem] * (sources + 1),
        scratch_shapes=[
            pltpu.VMEM(k_rows.shape, k_rows.dtype),
            pltpu.VMEM(v_rows.shape, v_rows.dtype),
            pltpu.VMEM((4 * (pages // LANES), LANES), f32),
            pltpu.VMEM((BLOCK, LANES), f32),
            pltpu.VMEM((8, BLOCK), f32),
            pltpu.VMEM((heads, BLOCK, LANES), f32),
            pltpu.VMEM((heads, BLOCK, 2 * LANES), f32),
            pltpu.VMEM((BLOCK, LANES), f32),
            pltpu.VMEM((LANES, BLOCK), f32),
            pltpu.VMEM((heads, requests, 2 * LANES), f32),
            pltpu.VMEM((heads, requests, LANES), f32),
            pltpu.SemaphoreType.DMA((2, pages // BLOCK)),
            pltpu.SemaphoreType.DMA((pieces,)),
        ],
        compiler_params=pltpu.CompilerParams(vmem_limit_bytes=46 * 1024 * 1024),
        name="attend",
    )(index, gathered, ks, vs, k_rows, v_rows, weight)


def in_vmem(arrays):
    return [pltpu.with_memory_space_constraint(a, pltpu.VMEM) for a in arrays]


def combine_kernel(*refs, heads):
    in_refs, out_ref = refs[:-1], refs[-1]
    width = heads * LANES
    aux = [ref[:, width:].astype(jnp.float32) for ref in in_refs]
    shift = [a[:, :heads] for a in aux]
    total = [a[:, heads : 2 * heads] + a[:, 2 * heads : 3 * heads] for a in aux]
    overall = functools.reduce(jnp.maximum, shift)
    factor = [jnp.exp2(a - overall) for a in shift]
    whole = sum(t * f for t, f in zip(total, factor))
    factor = [f / whole for f in factor]
    for h in range(heads):
        span = slice(h * LANES, (h + 1) * LANES)
        value = sum(
            ref[:, span].astype(jnp.float32) * f[:, h : h + 1] for ref, f in zip(in_refs, factor)
        )
        out_ref[:, span] = value.astype(jnp.bfloat16)


def combine(parts, heads):
    return pl.pallas_call(
        functools.partial(combine_kernel, heads=heads),
        in_specs=[pl.BlockSpec(memory_space=pltpu.VMEM)] * len(parts),
        out_shape=jax.ShapeDtypeStruct((parts[0].shape[0], heads * LANES), jnp.bfloat16),
        compiler_params=pltpu.CompilerParams(vmem_limit_bytes=24 * 1024 * 1024),
        name="combine",
    )(*parts[:1], *in_vmem(parts[1:]))


def project_kernel(x_ref, w_ref, *out_refs):
    for d, out_ref in enumerate(out_refs):
        out_ref[...] = jnp.dot(
            x_ref[...], w_ref[d], preferred_element_type=jnp.float32
        ).astype(jnp.bfloat16)


def project(x, weight):
    pieces, _, piece = weight.shape
    vmem = pl.BlockSpec(memory_space=pltpu.VMEM)
    return pl.pallas_call(
        project_kernel,
        out_shape=[jax.ShapeDtypeStruct((x.shape[0], piece), jnp.bfloat16)] * pieces,
        in_specs=[vmem, vmem],
        out_specs=[vmem] * pieces,
        compiler_params=pltpu.CompilerParams(vmem_limit_bytes=24 * 1024 * 1024),
        name="project",
    )(x, *in_vmem([weight]))


def exchange(parts, axis):
    count = len(parts)
    return [parts[0]] + [
        lax.ppermute(parts[d], axis, [(s, (s + d) % count) for s in range(count)])
        for d in range(1, count)
    ]


def pack_kernel(q_ref, len_ref, table_ref, out_ref, *, tokens):
    rows, heads, _ = q_ref.shape
    width = heads * LANES
    queries = jnp.transpose(q_ref[...].astype(jnp.float32), (1, 0, 2))
    for h in range(heads):
        out_ref[:, h * LANES : (h + 1) * LANES] = queries[h].astype(jnp.bfloat16)
    table = table_ref[...]
    out_ref[:, width : width + LANES] = (table >> 8).astype(jnp.float32).astype(jnp.bfloat16)
    out_ref[:, width + LANES : width + 2 * LANES] = (
        (table & 255).astype(jnp.float32).astype(jnp.bfloat16)
    )
    diagonal = lax.broadcasted_iota(jnp.int32, (rows, rows), 0) == lax.broadcasted_iota(
        jnp.int32, (rows, rows), 1
    )
    lengths = len_ref[...].astype(jnp.float32)
    length = jnp.sum(jnp.where(diagonal, lengths, 0.0), axis=1, keepdims=True)
    entry = lax.broadcasted_iota(jnp.int32, table.shape, 1).astype(jnp.float32)
    live = jnp.clip(length - entry * float(tokens), 0.0, float(tokens))
    out_ref[:, width + 2 * LANES :] = live.astype(jnp.bfloat16)


def pack_request(queries, lengths, page_table, tokens):
    rows, heads, _ = queries.shape
    page_table = jnp.pad(
        page_table, ((0, 0), (0, LANES - page_table.shape[1])), constant_values=-1
    )
    return pl.pallas_call(
        functools.partial(pack_kernel, tokens=tokens),
        out_shape=jax.ShapeDtypeStruct((rows, (heads + 3) * LANES), jnp.bfloat16),
        compiler_params=pltpu.CompilerParams(vmem_limit_bytes=24 * 1024 * 1024),
        name="pack",
    )(queries, lengths.reshape(1, rows), page_table)


def on_device(
    queries,
    k_codes,
    value_quantized_codes,
    key_page_scale,
    value_page_scale,
    lengths,
    page_table,
    out_weight,
):
    pages, tokens, kv, head_size = k_codes.shape
    rows, heads, _ = queries.shape
    sources = lax.axis_size("req")
    request = pack_request(queries, lengths, page_table, tokens)
    gathered = lax.all_gather(request, "req", axis=0, tiled=True)
    pieces = lax.axis_size("head")
    index = jnp.stack([lax.axis_index("req"), lax.axis_index("head")]).astype(jnp.int32)
    piece = out_weight.shape[1] // pieces
    *partial, weight = attend(
        gathered,
        index,
        k_codes.reshape(pages * tokens * kv, head_size),
        value_quantized_codes.reshape(pages * tokens * kv, head_size),
        key_page_scale.T,
        value_page_scale.T,
        out_weight,
        pieces if piece % LANES == 0 else 1,
        heads,
        kv,
        tokens,
        sources,
    )
    attention = combine(exchange(partial, "req"), heads)
    attention = lax.all_gather(attention, "req", axis=0, tiled=True)
    terms = project(attention, weight)
    if len(terms) < pieces:
        terms = [
            lax.dynamic_slice_in_dim(terms[0], ((index[1] + d) % pieces) * piece, piece, 1)
            for d in range(pieces)
        ]
    terms = exchange(terms, "head")
    return sum(t.astype(jnp.float32) for t in terms).astype(jnp.bfloat16)


def solution(mesh):
    in_specs = (
        P("req", "head", None),
        P("req", None, "head", None),
        P("req", None, "head", None),
        P("req", "head"),
        P("req", "head"),
        P("req"),
        P("req", None),
        P("head", "req"),
    )
    out_specs = P(None, ("req", "head"))
    return jax.shard_map(
        on_device, mesh=mesh, in_specs=in_specs, out_specs=out_specs, check_vma=False
    )
```

```python
import functools
import math

import jax
import jax.numpy as jnp
from jax import lax
from jax.experimental import pallas as pl
from jax.experimental.pallas import tpu as pltpu
from jax.sharding import PartitionSpec as P

floor_score = float(jnp.bfloat16(-1e30))
LANES = 128
GROUP = 8
BLOCK = 256


def place_pages(gath_ref, offset, pages, width, placed_ref):
    requests = gath_ref.shape[0]
    page_rows = pages // LANES
    chunk = 16
    line = lax.broadcasted_iota(jnp.int32, (chunk, LANES), 0)
    sub = lax.broadcasted_iota(jnp.int32, (LANES, LANES), 0)
    sub_row = lax.broadcasted_iota(jnp.int32, (page_rows, LANES), 0)

    def step(c, total):
        rows = pl.ds(pl.multiple_of(c * chunk, chunk), chunk)
        high = gath_ref[rows, width : width + LANES].astype(jnp.float32)
        low = gath_ref[rows, width + LANES : width + 2 * LANES].astype(jnp.float32)
        live = gath_ref[rows, width + 2 * LANES : width + 3 * LANES].astype(jnp.float32)
        slot = (high * 256.0 + low).astype(jnp.int32) - offset
        inside = (slot >= 0) & (slot < pages)
        slot_row = jnp.where(inside, slot >> 7, -1)
        slot_lane = slot & (LANES - 1)
        owner = c * chunk + line
        owner_high = (owner >> 7).astype(jnp.float32)
        owner_low = (owner & (LANES - 1)).astype(jnp.float32)
        for first in range(0, chunk, 2):
            lefts, rights = [], []
            for i in (first, first + 1):
                here = sub_row == slot_row[i : i + 1]
                parts = [
                    jnp.where(here, v[i : i + 1], 0.0) for v in (owner_high, owner_low, live, live)
                ]
                lefts.append(jnp.concatenate(parts, axis=0).astype(jnp.bfloat16))
                rights.append(
                    jnp.where(sub == slot_lane[i : i + 1], 1.0, 0.0).astype(jnp.bfloat16)
                )
            total += lax.dot_general(
                jnp.concatenate(lefts, axis=1),
                jnp.concatenate(rights, axis=1),
                (((1,), (1,)), ((), ())),
                preferred_element_type=jnp.float32,
            )
        return total

    start = jnp.zeros((4 * page_rows, LANES), jnp.float32)
    placed_ref[...] = lax.fori_loop(0, requests // chunk, step, start)


def attend_kernel(
    index_ref,
    gath_ref,
    ks_hbm,
    vs_hbm,
    k_hbm,
    v_hbm,
    w_hbm,
    *rest,
    heads,
    kv,
    tokens,
    sources,
):
    out_refs, w_out, scratch = rest[:sources], rest[sources], rest[sources + 1 :]
    (
        k_buf,
        v_buf,
        placed_ref,
        cols_ref,
        owner_ref,
        qg_ref,
        po_ref,
        pm_ref,
        pmt_ref,
        acc_ref,
        m_ref,
        ks_ref,
        vs_ref,
        sems,
        w_sems,
        scale_sems,
    ) = scratch
    requests = gath_ref.shape[0]
    width = heads * LANES
    pages = ks_hbm.shape[1]
    blocks = pages // BLOCK
    page_rows = pages // LANES
    halves = BLOCK // LANES
    block_rows = BLOCK * tokens * kv
    group_rows = GROUP * tokens * kv
    per_kv = heads // kv

    def copies(b):
        rows = pl.ds(b * block_rows, block_rows)
        return (
            pltpu.make_async_copy(k_hbm.at[rows], k_buf.at[rows], sems.at[0, b]),
            pltpu.make_async_copy(v_hbm.at[rows], v_buf.at[rows], sems.at[1, b]),
        )

    scale_copies = (
        pltpu.make_async_copy(ks_hbm, ks_ref, scale_sems.at[0]),
        pltpu.make_async_copy(vs_hbm, vs_ref, scale_sems.at[1]),
    )
    for copy in scale_copies:
        copy.start()
    pieces, _, piece = w_out.shape
    w_copies = []
    for d in range(pieces):
        at = pl.multiple_of(lax.rem(index_ref[1] + d, pieces) * piece, piece)
        w_copies.append(
            pltpu.make_async_copy(w_hbm.at[:, pl.ds(at, piece)], w_out.at[d], w_sems.at[d])
        )
    for b in range(blocks):
        for copy in copies(b):
            copy.start()
    for copy in w_copies:
        copy.start()

    place_pages(gath_ref, index_ref[0] * pages, pages, width, placed_ref)
    for copy in scale_copies:
        copy.wait()
    acc_ref[...] = jnp.zeros(acc_ref.shape, jnp.float32)
    m_ref[...] = jnp.full(m_ref.shape, floor_score, jnp.float32)

    col = lax.broadcasted_iota(jnp.int32, (GROUP, group_rows), 1)
    row = lax.broadcasted_iota(jnp.int32, (GROUP, group_rows), 0)
    token = (col % (tokens * kv)) // kv
    keys = [
        jnp.where((col // (tokens * kv) == row) & (col % kv == k), token, 2 * tokens).astype(
            jnp.float32
        )
        for k in range(kv)
    ]
    lane = lax.broadcasted_iota(jnp.int32, (GROUP, LANES), 1)
    sub8 = lax.broadcasted_iota(jnp.int32, (8, LANES), 0)
    lane_r = lax.broadcasted_iota(jnp.int32, (BLOCK, requests), 1).astype(jnp.float32)
    sub_r = lax.broadcasted_iota(jnp.int32, (requests, BLOCK), 0).astype(jnp.float32)
    ones = jnp.ones((group_rows, LANES), jnp.bfloat16)

    def block_step(b, carry):
        for u in range(halves):
            at = b * halves + u
            owner = placed_ref[pl.ds(at, 1), :] * 128.0 + placed_ref[pl.ds(page_rows + at, 1), :]
            live = placed_ref[pl.ds(2 * page_rows + at, 1), :]
            span = pl.ds(pl.multiple_of(at * LANES, LANES), LANES)
            rows = [owner, live]
            rows += [ks_ref[k : k + 1, span] * (math.log2(math.e) / math.sqrt(LANES)) for k in range(kv)]
            rows += [vs_ref[k : k + 1, span] for k in range(kv)]
            stacked = jnp.zeros((8, LANES), jnp.float32)
            for i, r in enumerate(rows):
                stacked = jnp.where(sub8 == i, r, stacked)
            full = jnp.concatenate([stacked, jnp.zeros((LANES - 8, LANES), jnp.float32)], axis=0)
            cols_ref[u * LANES : (u + 1) * LANES, :] = full.T
            owner_ref[0:1, u * LANES : (u + 1) * LANES] = owner
        member_t = jnp.where(cols_ref[:, 0:1] == lane_r, 1.0, 0.0).astype(jnp.bfloat16)
        for h in range(0, heads, 2):
            pair = jnp.dot(
                member_t,
                gath_ref[:, h * LANES : (h + 2) * LANES],
                preferred_element_type=jnp.float32,
            )
            qg_ref[h] = pair[:, :LANES]
            qg_ref[h + 1] = pair[:, LANES:]
        for copy in copies(b):
            copy.wait()

        def group_step(g, inner):
            at = pl.ds(pl.multiple_of(g * GROUP, GROUP), GROUP)
            start = pl.multiple_of(b * block_rows + g * group_rows, group_rows)
            q = qg_ref[:, at, :].reshape(heads * GROUP, LANES).astype(jnp.bfloat16)
            s = lax.dot_general(
                q,
                k_buf[pl.ds(start, group_rows), :],
                (((1,), (1,)), ((), ())),
                preferred_element_type=jnp.float32,
            ).reshape(heads, GROUP, group_rows)
            c = cols_ref[at, :]
            peaks = jnp.zeros((GROUP, LANES), jnp.float32)
            probs = []
            for k in range(kv):
                live = keys[k] < c[:, 1:2]
                scale = c[:, 2 + k : 3 + k]
                for i in range(k * per_kv, (k + 1) * per_kv):
                    sk = jnp.where(live, s[i] * scale, floor_score)
                    mx = jnp.max(sk, axis=-1, keepdims=True)
                    probs.append(jnp.exp2(sk - mx))
                    peaks = jnp.where(lane == i, mx, peaks)
            p = jnp.concatenate(probs, axis=0).astype(jnp.bfloat16)
            vg = jnp.concatenate([v_buf[pl.ds(start, group_rows), :], ones], axis=1)
            o = jnp.dot(p, vg, preferred_element_type=jnp.float32)
            o = o.reshape(heads, GROUP, 2 * LANES)
            for k in range(kv):
                hs = slice(k * per_kv, (k + 1) * per_kv)
                vscale = c[:, 2 + kv + k : 3 + kv + k]
                po_ref[hs, at, :LANES] = o[hs, :, :LANES] * vscale[None]
            po_ref[:, at, LANES:] = o[:, :, LANES:]
            pm_ref[at, :] = peaks
            return inner

        lax.fori_loop(0, BLOCK // GROUP, group_step, 0, unroll=8)
        for u in range(halves):
            span = slice(u * LANES, (u + 1) * LANES)
            pmt_ref[:, span] = pm_ref[span, :].T

        def head_step(h, inner):
            pm_row = pmt_ref[pl.ds(h, 1), :]
            member = sub_r == owner_ref[0:1, :]
            block_peak = jnp.max(
                jnp.where(member, pm_row, floor_score), axis=1, keepdims=True
            )
            old = m_ref[h]
            new = jnp.maximum(old, block_peak)
            alpha = jnp.exp2(old - new)
            wide = jnp.concatenate([new] * halves, axis=1)
            w = jnp.exp2(jnp.where(member, pm_row - wide, floor_score)).astype(jnp.bfloat16)
            o = jnp.dot(w, po_ref[h].astype(jnp.bfloat16), preferred_element_type=jnp.float32)
            acc_ref[h] = acc_ref[h] * jnp.concatenate([alpha, alpha], axis=1) + o
            m_ref[h] = new
            return inner

        lax.fori_loop(0, heads, head_step, 0, unroll=8)
        return carry

    lax.fori_loop(0, blocks, block_step, 0)

    rows = requests // sources
    lane_out = lax.broadcasted_iota(jnp.int32, (rows, LANES), 1)
    for d in range(sources):
        target = lax.rem(index_ref[0] + d, sources)
        here = pl.ds(pl.multiple_of(target * rows, rows), rows)
        aux = jnp.zeros((rows, LANES), jnp.float32)
        for h in range(heads):
            peak = m_ref[h, here, :]
            shift = peak.astype(jnp.bfloat16).astype(jnp.float32)
            factor = jnp.exp2(peak - shift)
            out_refs[d][:, h * LANES : (h + 1) * LANES] = (
                acc_ref[h, here, :LANES] * factor
            ).astype(jnp.bfloat16)
            total = acc_ref[h, here, LANES:] * factor
            total_high = total.astype(jnp.bfloat16).astype(jnp.float32)
            aux = jnp.where(lane_out == h, shift, aux)
            aux = jnp.where(lane_out == heads + h, total_high, aux)
            aux = jnp.where(lane_out == 2 * heads + h, total - total_high, aux)
        out_refs[d][:, width : width + LANES] = aux.astype(jnp.bfloat16)
    for copy in w_copies:
        copy.wait()


def attend(gathered, index, k_rows, v_rows, ks, vs, weight, pieces, heads, kv, tokens, sources):
    depth, columns = weight.shape
    requests = gathered.shape[0]
    pages = ks.shape[1]
    f32 = jnp.float32
    vmem = pl.BlockSpec(memory_space=pltpu.VMEM)
    hbm = pl.BlockSpec(memory_space=pltpu.HBM)
    return pl.pallas_call(
        functools.partial(attend_kernel, heads=heads, kv=kv, tokens=tokens, sources=sources),
        out_shape=[
            jax.ShapeDtypeStruct((requests // sources, (heads + 1) * LANES), jnp.bfloat16)
        ]
        * sources
        + [pltpu.VMEM((pieces, depth, columns // pieces), weight.dtype)],
        in_specs=[pl.BlockSpec(memory_space=pltpu.SMEM), vmem, hbm, hbm, hbm, hbm, hbm],
        out_specs=[vmem] * (sources + 1),
        scratch_shapes=[
            pltpu.VMEM(k_rows.shape, k_rows.dtype),
            pltpu.VMEM(v_rows.shape, v_rows.dtype),
            pltpu.VMEM((4 * (pages // LANES), LANES), f32),
            pltpu.VMEM((BLOCK, LANES), f32),
            pltpu.VMEM((8, BLOCK), f32),
            pltpu.VMEM((heads, BLOCK, LANES), f32),
            pltpu.VMEM((heads, BLOCK, 2 * LANES), f32),
            pltpu.VMEM((BLOCK, LANES), f32),
            pltpu.VMEM((LANES, BLOCK), f32),
            pltpu.VMEM((heads, requests, 2 * LANES), f32),
            pltpu.VMEM((heads, requests, LANES), f32),
            pltpu.VMEM(ks.shape, f32),
            pltpu.VMEM(vs.shape, f32),
            pltpu.SemaphoreType.DMA((2, pages // BLOCK)),
            pltpu.SemaphoreType.DMA((pieces,)),
            pltpu.SemaphoreType.DMA((2,)),
        ],
        compiler_params=pltpu.CompilerParams(vmem_limit_bytes=46 * 1024 * 1024),
        name="attend",
    )(index, *in_vmem([gathered]), *in_hbm([ks, vs]), k_rows, v_rows, weight)


def in_hbm(arrays):
    return [pltpu.with_memory_space_constraint(a, pltpu.HBM) for a in arrays]


def in_vmem(arrays):
    return [pltpu.with_memory_space_constraint(a, pltpu.VMEM) for a in arrays]


def combine_kernel(*refs, heads):
    in_refs, out_ref = refs[:-1], refs[-1]
    width = heads * LANES
    aux = [ref[:, width:].astype(jnp.float32) for ref in in_refs]
    shift = [a[:, :heads] for a in aux]
    total = [a[:, heads : 2 * heads] + a[:, 2 * heads : 3 * heads] for a in aux]
    overall = functools.reduce(jnp.maximum, shift)
    factor = [jnp.exp2(a - overall) for a in shift]
    whole = sum(t * f for t, f in zip(total, factor))
    factor = [f / whole for f in factor]
    for h in range(heads):
        span = slice(h * LANES, (h + 1) * LANES)
        value = sum(
            ref[:, span].astype(jnp.float32) * f[:, h : h + 1] for ref, f in zip(in_refs, factor)
        )
        out_ref[:, span] = value.astype(jnp.bfloat16)


def combine(parts, heads):
    return pl.pallas_call(
        functools.partial(combine_kernel, heads=heads),
        in_specs=[pl.BlockSpec(memory_space=pltpu.VMEM)] * len(parts),
        out_shape=jax.ShapeDtypeStruct((parts[0].shape[0], heads * LANES), jnp.bfloat16),
        compiler_params=pltpu.CompilerParams(vmem_limit_bytes=24 * 1024 * 1024),
        name="combine",
    )(*parts[:1], *in_vmem(parts[1:]))


def project_kernel(x_ref, w_ref, *out_refs):
    for d, out_ref in enumerate(out_refs):
        out_ref[...] = jnp.dot(
            x_ref[...], w_ref[d], preferred_element_type=jnp.float32
        ).astype(jnp.bfloat16)


def project(x, weight):
    pieces, _, piece = weight.shape
    vmem = pl.BlockSpec(memory_space=pltpu.VMEM)
    return pl.pallas_call(
        project_kernel,
        out_shape=[jax.ShapeDtypeStruct((x.shape[0], piece), jnp.bfloat16)] * pieces,
        in_specs=[vmem, vmem],
        out_specs=[vmem] * pieces,
        compiler_params=pltpu.CompilerParams(vmem_limit_bytes=24 * 1024 * 1024),
        name="project",
    )(x, *in_vmem([weight]))


def exchange(parts, axis):
    count = len(parts)
    return [parts[0]] + [
        lax.ppermute(parts[d], axis, [(s, (s + d) % count) for s in range(count)])
        for d in range(1, count)
    ]


def pack_kernel(q_hbm, len_hbm, table_hbm, out_ref, q_ref, len_ref, table_ref, sems, *, tokens):
    copies = [
        pltpu.make_async_copy(source, target, sems.at[i])
        for i, (source, target) in enumerate(
            ((q_hbm, q_ref), (len_hbm, len_ref), (table_hbm, table_ref))
        )
    ]
    for copy in copies:
        copy.start()
    for copy in copies:
        copy.wait()
    rows, heads, _ = q_ref.shape
    width = heads * LANES
    queries = jnp.transpose(q_ref[...].astype(jnp.float32), (1, 0, 2))
    for h in range(heads):
        out_ref[:, h * LANES : (h + 1) * LANES] = queries[h].astype(jnp.bfloat16)
    table = table_ref[...]
    out_ref[:, width : width + LANES] = (table >> 8).astype(jnp.float32).astype(jnp.bfloat16)
    out_ref[:, width + LANES : width + 2 * LANES] = (
        (table & 255).astype(jnp.float32).astype(jnp.bfloat16)
    )
    diagonal = lax.broadcasted_iota(jnp.int32, (rows, rows), 0) == lax.broadcasted_iota(
        jnp.int32, (rows, rows), 1
    )
    lengths = len_ref[...].astype(jnp.float32)
    length = jnp.sum(jnp.where(diagonal, lengths, 0.0), axis=1, keepdims=True)
    entry = lax.broadcasted_iota(jnp.int32, table.shape, 1).astype(jnp.float32)
    live = jnp.clip(length - entry * float(tokens), 0.0, float(tokens))
    out_ref[:, width + 2 * LANES :] = live.astype(jnp.bfloat16)


def pack_request(queries, lengths, page_table, tokens):
    rows, heads, _ = queries.shape
    if page_table.shape[1] < LANES:
        spare = ((0, 0), (0, LANES - page_table.shape[1]))
        page_table = jnp.pad(page_table, spare, constant_values=-1)
    return pl.pallas_call(
        functools.partial(pack_kernel, tokens=tokens),
        out_shape=jax.ShapeDtypeStruct((rows, (heads + 3) * LANES), jnp.bfloat16),
        in_specs=[pl.BlockSpec(memory_space=pltpu.HBM)] * 3,
        scratch_shapes=[
            pltpu.VMEM(queries.shape, queries.dtype),
            pltpu.VMEM((1, rows), jnp.int32),
            pltpu.VMEM(page_table.shape, jnp.int32),
            pltpu.SemaphoreType.DMA((3,)),
        ],
        compiler_params=pltpu.CompilerParams(vmem_limit_bytes=24 * 1024 * 1024),
        name="pack",
    )(*in_hbm([queries, lengths.reshape(1, rows), page_table]))


def on_device(
    queries,
    k_codes,
    value_quantized_codes,
    key_page_scale,
    value_page_scale,
    lengths,
    page_table,
    out_weight,
):
    pages, tokens, kv, head_size = k_codes.shape
    rows, heads, _ = queries.shape
    sources = lax.axis_size("req")
    request = pack_request(queries, lengths, page_table, tokens)
    gathered = lax.all_gather(request, "req", axis=0, tiled=True)
    pieces = lax.axis_size("head")
    index = jnp.stack([lax.axis_index("req"), lax.axis_index("head")]).astype(jnp.int32)
    piece = out_weight.shape[1] // pieces
    *partial, weight = attend(
        gathered,
        index,
        k_codes.reshape(pages * tokens * kv, head_size),
        value_quantized_codes.reshape(pages * tokens * kv, head_size),
        key_page_scale.T,
        value_page_scale.T,
        out_weight,
        pieces if piece % LANES == 0 else 1,
        heads,
        kv,
        tokens,
        sources,
    )
    attention = combine(exchange(partial, "req"), heads)
    attention = lax.all_gather(attention, "req", axis=0, tiled=True)
    terms = project(attention, weight)
    if len(terms) < pieces:
        terms = [
            lax.dynamic_slice_in_dim(terms[0], ((index[1] + d) % pieces) * piece, piece, 1)
            for d in range(pieces)
        ]
    terms = exchange(terms, "head")
    return sum(t.astype(jnp.float32) for t in terms).astype(jnp.bfloat16)


def solution(mesh):
    in_specs = (
        P("req", "head", None),
        P("req", None, "head", None),
        P("req", None, "head", None),
        P("req", "head"),
        P("req", "head"),
        P("req"),
        P("req", None),
        P("head", "req"),
    )
    out_specs = P(None, ("req", "head"))
    return jax.shard_map(
        on_device, mesh=mesh, in_specs=in_specs, out_specs=out_specs, check_vma=False
    )
```

```python
import functools
import math

import jax
import jax.numpy as jnp
from jax import lax
from jax.experimental import pallas as pl
from jax.experimental.pallas import tpu as pltpu
from jax.sharding import PartitionSpec as P

floor_score = float(jnp.bfloat16(-1e30))
LANES = 128
GROUP = 8
BLOCK = 256


def place_pages(gath_ref, offset, pages, width, placed_ref):
    requests = gath_ref.shape[0]
    page_rows = pages // LANES
    chunk = 16
    line = lax.broadcasted_iota(jnp.int32, (chunk, LANES), 0)
    sub = lax.broadcasted_iota(jnp.int32, (LANES, LANES), 0)
    sub_row = lax.broadcasted_iota(jnp.int32, (page_rows, LANES), 0)

    def step(c, total):
        rows = pl.ds(pl.multiple_of(c * chunk, chunk), chunk)
        high = gath_ref[rows, width : width + LANES].astype(jnp.float32)
        low = gath_ref[rows, width + LANES : width + 2 * LANES].astype(jnp.float32)
        live = gath_ref[rows, width + 2 * LANES : width + 3 * LANES].astype(jnp.float32)
        slot = (high * 256.0 + low).astype(jnp.int32) - offset
        inside = (slot >= 0) & (slot < pages)
        slot_row = jnp.where(inside, slot >> 7, -1)
        slot_lane = slot & (LANES - 1)
        owner = c * chunk + line
        owner_high = (owner >> 7).astype(jnp.float32)
        owner_low = (owner & (LANES - 1)).astype(jnp.float32)
        for first in range(0, chunk, 2):
            lefts, rights = [], []
            for i in (first, first + 1):
                here = sub_row == slot_row[i : i + 1]
                parts = [
                    jnp.where(here, v[i : i + 1], 0.0) for v in (owner_high, owner_low, live, live)
                ]
                lefts.append(jnp.concatenate(parts, axis=0).astype(jnp.bfloat16))
                rights.append(
                    jnp.where(sub == slot_lane[i : i + 1], 1.0, 0.0).astype(jnp.bfloat16)
                )
            total += lax.dot_general(
                jnp.concatenate(lefts, axis=1),
                jnp.concatenate(rights, axis=1),
                (((1,), (1,)), ((), ())),
                preferred_element_type=jnp.float32,
            )
        return total

    start = jnp.zeros((4 * page_rows, LANES), jnp.float32)
    placed_ref[...] = lax.fori_loop(0, requests // chunk, step, start)


def attend_kernel(
    index_ref,
    gath_ref,
    ks_hbm,
    vs_hbm,
    k_hbm,
    v_hbm,
    w_hbm,
    *rest,
    heads,
    kv,
    tokens,
    sources,
):
    out_refs, w_out, scratch = rest[:sources], rest[sources], rest[sources + 1 :]
    (
        k_buf,
        v_buf,
        placed_ref,
        cols_ref,
        owner_ref,
        qg_ref,
        po_ref,
        pm_ref,
        pmt_ref,
        acc_ref,
        m_ref,
        ks_ref,
        vs_ref,
        sems,
        w_sems,
        scale_sems,
    ) = scratch
    requests = gath_ref.shape[0]
    width = heads * LANES
    pages = ks_hbm.shape[1]
    blocks = pages // BLOCK
    page_rows = pages // LANES
    halves = BLOCK // LANES
    block_rows = BLOCK * tokens * kv
    group_rows = GROUP * tokens * kv
    per_kv = heads // kv

    def copies(b):
        rows = pl.ds(b * block_rows, block_rows)
        return (
            pltpu.make_async_copy(k_hbm.at[rows], k_buf.at[rows], sems.at[0, b]),
            pltpu.make_async_copy(v_hbm.at[rows], v_buf.at[rows], sems.at[1, b]),
        )

    scale_copies = (
        pltpu.make_async_copy(ks_hbm, ks_ref, scale_sems.at[0]),
        pltpu.make_async_copy(vs_hbm, vs_ref, scale_sems.at[1]),
    )
    for copy in scale_copies:
        copy.start()
    pieces, _, piece = w_out.shape
    w_copies = []
    for d in range(pieces):
        at = pl.multiple_of(lax.rem(index_ref[1] + d, pieces) * piece, piece)
        w_copies.append(
            pltpu.make_async_copy(w_hbm.at[:, pl.ds(at, piece)], w_out.at[d], w_sems.at[d])
        )
    for b in range(blocks):
        for copy in copies(b):
            copy.start()
    for copy in w_copies:
        copy.start()

    place_pages(gath_ref, index_ref[0] * pages, pages, width, placed_ref)
    for copy in scale_copies:
        copy.wait()
    acc_ref[...] = jnp.zeros(acc_ref.shape, jnp.float32)
    m_ref[...] = jnp.full(m_ref.shape, floor_score, jnp.float32)

    col = lax.broadcasted_iota(jnp.int32, (GROUP, group_rows), 1)
    row = lax.broadcasted_iota(jnp.int32, (GROUP, group_rows), 0)
    token = (col % (tokens * kv)) // kv
    keys = [
        jnp.where((col // (tokens * kv) == row) & (col % kv == k), token, 2 * tokens).astype(
            jnp.float32
        )
        for k in range(kv)
    ]
    lane = lax.broadcasted_iota(jnp.int32, (GROUP, LANES), 1)
    sub8 = lax.broadcasted_iota(jnp.int32, (8, LANES), 0)
    lane_r = lax.broadcasted_iota(jnp.int32, (BLOCK, requests), 1).astype(jnp.float32)
    sub_r = lax.broadcasted_iota(jnp.int32, (requests, BLOCK), 0).astype(jnp.float32)
    ones = jnp.ones((group_rows, LANES), jnp.bfloat16)

    def block_step(b, carry):
        for u in range(halves):
            at = b * halves + u
            owner = placed_ref[pl.ds(at, 1), :] * 128.0 + placed_ref[pl.ds(page_rows + at, 1), :]
            live = placed_ref[pl.ds(2 * page_rows + at, 1), :]
            span = pl.ds(pl.multiple_of(at * LANES, LANES), LANES)
            rows = [owner, live]
            rows += [ks_ref[k : k + 1, span] * (math.log2(math.e) / math.sqrt(LANES)) for k in range(kv)]
            rows += [vs_ref[k : k + 1, span] for k in range(kv)]
            stacked = jnp.zeros((8, LANES), jnp.float32)
            for i, r in enumerate(rows):
                stacked = jnp.where(sub8 == i, r, stacked)
            full = jnp.concatenate([stacked, jnp.zeros((LANES - 8, LANES), jnp.float32)], axis=0)
            cols_ref[u * LANES : (u + 1) * LANES, :] = full.T
            owner_ref[0:1, u * LANES : (u + 1) * LANES] = owner
        member_t = jnp.where(cols_ref[:, 0:1] == lane_r, 1.0, 0.0).astype(jnp.bfloat16)
        for h in range(0, heads, 2):
            pair = jnp.dot(
                member_t,
                gath_ref[:, h * LANES : (h + 2) * LANES],
                preferred_element_type=jnp.float32,
            )
            qg_ref[h] = pair[:, :LANES]
            qg_ref[h + 1] = pair[:, LANES:]
        for copy in copies(b):
            copy.wait()

        def group_step(g, inner):
            at = pl.ds(pl.multiple_of(g * GROUP, GROUP), GROUP)
            start = pl.multiple_of(b * block_rows + g * group_rows, group_rows)
            q = qg_ref[:, at, :].reshape(heads * GROUP, LANES).astype(jnp.bfloat16)
            s = lax.dot_general(
                q,
                k_buf[pl.ds(start, group_rows), :],
                (((1,), (1,)), ((), ())),
                preferred_element_type=jnp.float32,
            ).reshape(heads, GROUP, group_rows)
            c = cols_ref[at, :]
            peaks = jnp.zeros((GROUP, LANES), jnp.float32)
            probs = []
            for k in range(kv):
                live = keys[k] < c[:, 1:2]
                scale = c[:, 2 + k : 3 + k]
                for i in range(k * per_kv, (k + 1) * per_kv):
                    sk = jnp.where(live, s[i] * scale, floor_score)
                    mx = jnp.max(sk, axis=-1, keepdims=True)
                    probs.append(jnp.exp2(sk - mx))
                    peaks = jnp.where(lane == i, mx, peaks)
            p = jnp.concatenate(probs, axis=0).astype(jnp.bfloat16)
            vg = jnp.concatenate([v_buf[pl.ds(start, group_rows), :], ones], axis=1)
            o = jnp.dot(p, vg, preferred_element_type=jnp.float32)
            o = o.reshape(heads, GROUP, 2 * LANES)
            for k in range(kv):
                hs = slice(k * per_kv, (k + 1) * per_kv)
                vscale = c[:, 2 + kv + k : 3 + kv + k]
                po_ref[hs, at, :LANES] = o[hs, :, :LANES] * vscale[None]
            po_ref[:, at, LANES:] = o[:, :, LANES:]
            pm_ref[at, :] = peaks
            return inner

        lax.fori_loop(0, BLOCK // GROUP, group_step, 0, unroll=8)
        for u in range(halves):
            span = slice(u * LANES, (u + 1) * LANES)
            pmt_ref[:, span] = pm_ref[span, :].T

        def head_step(h, inner):
            pm_row = pmt_ref[pl.ds(h, 1), :]
            member = sub_r == owner_ref[0:1, :]
            block_peak = jnp.max(
                jnp.where(member, pm_row, floor_score), axis=1, keepdims=True
            )
            old = m_ref[h]
            new = jnp.maximum(old, block_peak)
            alpha = jnp.exp2(old - new)
            wide = jnp.concatenate([new] * halves, axis=1)
            w = jnp.exp2(jnp.where(member, pm_row - wide, floor_score)).astype(jnp.bfloat16)
            o = jnp.dot(w, po_ref[h].astype(jnp.bfloat16), preferred_element_type=jnp.float32)
            acc_ref[h] = acc_ref[h] * jnp.concatenate([alpha, alpha], axis=1) + o
            m_ref[h] = new
            return inner

        lax.fori_loop(0, heads, head_step, 0, unroll=4)
        return carry

    lax.fori_loop(0, blocks, block_step, 0)

    rows = requests // sources
    lane_out = lax.broadcasted_iota(jnp.int32, (rows, LANES), 1)
    for d in range(sources):
        target = lax.rem(index_ref[0] + d, sources)
        here = pl.ds(pl.multiple_of(target * rows, rows), rows)
        aux = jnp.zeros((rows, LANES), jnp.float32)
        for h in range(heads):
            peak = m_ref[h, here, :]
            shift = peak.astype(jnp.bfloat16).astype(jnp.float32)
            factor = jnp.exp2(peak - shift)
            out_refs[d][:, h * LANES : (h + 1) * LANES] = (
                acc_ref[h, here, :LANES] * factor
            ).astype(jnp.bfloat16)
            total = acc_ref[h, here, LANES:] * factor
            total_high = total.astype(jnp.bfloat16).astype(jnp.float32)
            aux = jnp.where(lane_out == h, shift, aux)
            aux = jnp.where(lane_out == heads + h, total_high, aux)
            aux = jnp.where(lane_out == 2 * heads + h, total - total_high, aux)
        out_refs[d][:, width : width + LANES] = aux.astype(jnp.bfloat16)
    for copy in w_copies:
        copy.wait()


def attend(gathered, index, k_rows, v_rows, ks, vs, weight, pieces, heads, kv, tokens, sources):
    depth, columns = weight.shape
    requests = gathered.shape[0]
    pages = ks.shape[1]
    f32 = jnp.float32
    vmem = pl.BlockSpec(memory_space=pltpu.VMEM)
    hbm = pl.BlockSpec(memory_space=pltpu.HBM)
    return pl.pallas_call(
        functools.partial(attend_kernel, heads=heads, kv=kv, tokens=tokens, sources=sources),
        out_shape=[
            jax.ShapeDtypeStruct((requests // sources, (heads + 1) * LANES), jnp.bfloat16)
        ]
        * sources
        + [pltpu.VMEM((pieces, depth, columns // pieces), weight.dtype)],
        in_specs=[pl.BlockSpec(memory_space=pltpu.SMEM), vmem, hbm, hbm, hbm, hbm, hbm],
        out_specs=[vmem] * (sources + 1),
        scratch_shapes=[
            pltpu.VMEM(k_rows.shape, k_rows.dtype),
            pltpu.VMEM(v_rows.shape, v_rows.dtype),
            pltpu.VMEM((4 * (pages // LANES), LANES), f32),
            pltpu.VMEM((BLOCK, LANES), f32),
            pltpu.VMEM((8, BLOCK), f32),
            pltpu.VMEM((heads, BLOCK, LANES), f32),
            pltpu.VMEM((heads, BLOCK, 2 * LANES), f32),
            pltpu.VMEM((BLOCK, LANES), f32),
            pltpu.VMEM((LANES, BLOCK), f32),
            pltpu.VMEM((heads, requests, 2 * LANES), f32),
            pltpu.VMEM((heads, requests, LANES), f32),
            pltpu.VMEM(ks.shape, f32),
            pltpu.VMEM(vs.shape, f32),
            pltpu.SemaphoreType.DMA((2, pages // BLOCK)),
            pltpu.SemaphoreType.DMA((pieces,)),
            pltpu.SemaphoreType.DMA((2,)),
        ],
        compiler_params=pltpu.CompilerParams(vmem_limit_bytes=46 * 1024 * 1024),
        name="attend",
    )(index, *in_vmem([gathered]), *in_hbm([ks, vs]), k_rows, v_rows, weight)


def in_hbm(arrays):
    return [pltpu.with_memory_space_constraint(a, pltpu.HBM) for a in arrays]


def in_vmem(arrays):
    return [pltpu.with_memory_space_constraint(a, pltpu.VMEM) for a in arrays]


def combine_kernel(*refs, heads):
    in_refs, out_ref = refs[:-1], refs[-1]
    width = heads * LANES
    aux = [ref[:, width:].astype(jnp.float32) for ref in in_refs]
    shift = [a[:, :heads] for a in aux]
    total = [a[:, heads : 2 * heads] + a[:, 2 * heads : 3 * heads] for a in aux]
    overall = functools.reduce(jnp.maximum, shift)
    factor = [jnp.exp2(a - overall) for a in shift]
    whole = sum(t * f for t, f in zip(total, factor))
    factor = [f / whole for f in factor]
    for h in range(heads):
        span = slice(h * LANES, (h + 1) * LANES)
        value = sum(
            ref[:, span].astype(jnp.float32) * f[:, h : h + 1] for ref, f in zip(in_refs, factor)
        )
        out_ref[:, span] = value.astype(jnp.bfloat16)


def combine(parts, heads):
    return pl.pallas_call(
        functools.partial(combine_kernel, heads=heads),
        in_specs=[pl.BlockSpec(memory_space=pltpu.VMEM)] * len(parts),
        out_shape=jax.ShapeDtypeStruct((parts[0].shape[0], heads * LANES), jnp.bfloat16),
        compiler_params=pltpu.CompilerParams(vmem_limit_bytes=24 * 1024 * 1024),
        name="combine",
    )(*parts[:1], *in_vmem(parts[1:]))


def project_kernel(x_ref, w_ref, *out_refs):
    for d, out_ref in enumerate(out_refs):
        out_ref[...] = jnp.dot(
            x_ref[...], w_ref[d], preferred_element_type=jnp.float32
        ).astype(jnp.bfloat16)


def project(x, weight):
    pieces, _, piece = weight.shape
    vmem = pl.BlockSpec(memory_space=pltpu.VMEM)
    return pl.pallas_call(
        project_kernel,
        out_shape=[jax.ShapeDtypeStruct((x.shape[0], piece), jnp.bfloat16)] * pieces,
        in_specs=[vmem, vmem],
        out_specs=[vmem] * pieces,
        compiler_params=pltpu.CompilerParams(vmem_limit_bytes=24 * 1024 * 1024),
        name="project",
    )(x, *in_vmem([weight]))


def exchange(parts, axis):
    count = len(parts)
    return [parts[0]] + [
        lax.ppermute(parts[d], axis, [(s, (s + d) % count) for s in range(count)])
        for d in range(1, count)
    ]


def pack_kernel(q_hbm, len_hbm, table_hbm, out_ref, q_ref, len_ref, table_ref, sems, *, tokens):
    copies = [
        pltpu.make_async_copy(source, target, sems.at[i])
        for i, (source, target) in enumerate(
            ((q_hbm, q_ref), (len_hbm, len_ref), (table_hbm, table_ref))
        )
    ]
    for copy in copies:
        copy.start()
    for copy in copies:
        copy.wait()
    rows, heads, _ = q_ref.shape
    width = heads * LANES
    queries = jnp.transpose(q_ref[...].astype(jnp.float32), (1, 0, 2))
    for h in range(heads):
        out_ref[:, h * LANES : (h + 1) * LANES] = queries[h].astype(jnp.bfloat16)
    table = table_ref[...]
    out_ref[:, width : width + LANES] = (table >> 8).astype(jnp.float32).astype(jnp.bfloat16)
    out_ref[:, width + LANES : width + 2 * LANES] = (
        (table & 255).astype(jnp.float32).astype(jnp.bfloat16)
    )
    diagonal = lax.broadcasted_iota(jnp.int32, (rows, rows), 0) == lax.broadcasted_iota(
        jnp.int32, (rows, rows), 1
    )
    lengths = len_ref[...].astype(jnp.float32)
    length = jnp.sum(jnp.where(diagonal, lengths, 0.0), axis=1, keepdims=True)
    entry = lax.broadcasted_iota(jnp.int32, table.shape, 1).astype(jnp.float32)
    live = jnp.clip(length - entry * float(tokens), 0.0, float(tokens))
    out_ref[:, width + 2 * LANES :] = live.astype(jnp.bfloat16)


def pack_request(queries, lengths, page_table, tokens):
    rows, heads, _ = queries.shape
    if page_table.shape[1] < LANES:
        spare = ((0, 0), (0, LANES - page_table.shape[1]))
        page_table = jnp.pad(page_table, spare, constant_values=-1)
    return pl.pallas_call(
        functools.partial(pack_kernel, tokens=tokens),
        out_shape=jax.ShapeDtypeStruct((rows, (heads + 3) * LANES), jnp.bfloat16),
        in_specs=[pl.BlockSpec(memory_space=pltpu.HBM)] * 3,
        scratch_shapes=[
            pltpu.VMEM(queries.shape, queries.dtype),
            pltpu.VMEM((1, rows), jnp.int32),
            pltpu.VMEM(page_table.shape, jnp.int32),
            pltpu.SemaphoreType.DMA((3,)),
        ],
        compiler_params=pltpu.CompilerParams(vmem_limit_bytes=24 * 1024 * 1024),
        name="pack",
    )(*in_hbm([queries, lengths.reshape(1, rows), page_table]))


def on_device(
    queries,
    k_codes,
    value_quantized_codes,
    key_page_scale,
    value_page_scale,
    lengths,
    page_table,
    out_weight,
):
    pages, tokens, kv, head_size = k_codes.shape
    rows, heads, _ = queries.shape
    sources = lax.axis_size("req")
    request = pack_request(queries, lengths, page_table, tokens)
    gathered = lax.all_gather(request, "req", axis=0, tiled=True)
    pieces = lax.axis_size("head")
    index = jnp.stack([lax.axis_index("req"), lax.axis_index("head")]).astype(jnp.int32)
    piece = out_weight.shape[1] // pieces
    *partial, weight = attend(
        gathered,
        index,
        k_codes.reshape(pages * tokens * kv, head_size),
        value_quantized_codes.reshape(pages * tokens * kv, head_size),
        key_page_scale.T,
        value_page_scale.T,
        out_weight,
        pieces if piece % LANES == 0 else 1,
        heads,
        kv,
        tokens,
        sources,
    )
    attention = combine(exchange(partial, "req"), heads)
    attention = lax.all_gather(attention, "req", axis=0, tiled=True)
    terms = project(attention, weight)
    if len(terms) < pieces:
        terms = [
            lax.dynamic_slice_in_dim(terms[0], ((index[1] + d) % pieces) * piece, piece, 1)
            for d in range(pieces)
        ]
    terms = exchange(terms, "head")
    return sum(t.astype(jnp.float32) for t in terms).astype(jnp.bfloat16)


def solution(mesh):
    in_specs = (
        P("req", "head", None),
        P("req", None, "head", None),
        P("req", None, "head", None),
        P("req", "head"),
        P("req", "head"),
        P("req"),
        P("req", None),
        P("head", "req"),
    )
    out_specs = P(None, ("req", "head"))
    return jax.shard_map(
        on_device, mesh=mesh, in_specs=in_specs, out_specs=out_specs, check_vma=False
    )
```
